256 devices in a mesh: dp: 8 (over x, core), tensor: 32 (over z, y).
Axes of the slice: x: 4, y: 4, z: 8, core: 2. Of those that a mesh axis runs over, the one named last changes fastest.
Arguments:
- hidden: bfloat16 [6144, 4096], P('dp', 'tensor'), may hold values from -2000 to 2000
- out_embed: bfloat16 [65536, 4096], P('tensor', 'dp'), may hold values from -0.3 to 0.3
- labels: int32 [6144], P('dp'), may hold values from 0 to 65535
Outputs:
- token_loss: float32 [6144], P(('dp', 'tensor'))
- mean_loss: float32 [], replicated
The draws below stay inside these ranges and needn't reach their ends.
All inputs are finite; a program needn't handle non-finite values.
Results may differ from the reference program's by a relative error of at most 0.0003.
Values may be sent and summed in bfloat16 or wider, within the bound.
A program may use at most 128 MiB of HBM per device.

```python
import math
import jax
import jax.numpy as jnp
import numpy as np
from jax import lax

D = 4096
VOCAB = 65536
TOKENS = 6144


def embed_values(key):
    embed_key = jax.random.fold_in(key, 7)
    values = jnp.clip(jax.random.normal(embed_key, (VOCAB, D), jnp.float32) * 0.05, -0.3, 0.3)
    return values.astype(jnp.bfloat16).astype(jnp.float32)


def draw_out_embed(key, part):
    return embed_values(key).astype(jnp.bfloat16)


def draw_hidden(key, part):
    noise_key = jax.random.fold_in(jax.random.fold_in(key, 11), 0)
    pick_key = jax.random.fold_in(jax.random.fold_in(key, 11), 2)
    first_key = jax.random.fold_in(jax.random.fold_in(key, 11), 3)
    second_key = jax.random.fold_in(jax.random.fold_in(key, 11), 4)
    power_key = jax.random.fold_in(jax.random.fold_in(key, 11), 5)
    gap_key = jax.random.fold_in(jax.random.fold_in(key, 11), 6)
    values = jnp.clip(jax.random.normal(noise_key, (TOKENS, D), jnp.float32), -6.0, 6.0)
    embed = embed_values(key)
    chosen = jax.random.randint(pick_key, (TOKENS,), 0, 12) == 0
    first_row = jax.random.randint(first_key, (TOKENS,), 0, VOCAB)
    second_row = (first_row + 1 + jax.random.randint(second_key, (TOKENS,), 0, VOCAB - 1)) % VOCAB
    strength = jax.random.uniform(power_key, (TOKENS,), jnp.float32, 100.0, 320.0)
    gap = jax.random.uniform(gap_key, (TOKENS,), jnp.float32, 1.0, 3.0)
    first_vec = embed[first_row]
    second_vec = embed[second_row]
    g11 = jnp.sum(first_vec * first_vec, axis=1)
    g22 = jnp.sum(second_vec * second_vec, axis=1)
    g12 = jnp.sum(first_vec * second_vec, axis=1)
    det = g11 * g22 - g12 * g12
    target_one = strength
    target_two = strength - gap
    coef_one = (g22 * target_one - g12 * target_two) / det
    coef_two = (g11 * target_two - g12 * target_one) / det
    aligned = coef_one[:, None] * first_vec + coef_two[:, None] * second_vec
    aligned = jnp.clip(aligned, -2000.0, 2000.0)
    values = jnp.where(chosen[:, None], aligned, values)
    return values.astype(jnp.bfloat16)


def set_ends(values, own_key, least, high):
    longest = values.shape.index(max(values.shape))
    spots = []
    for shift in (0, 1):
        where = [jax.random.randint(jax.random.fold_in(own_key, axis), (), 0, length) for axis, length in enumerate(values.shape)]
        where[longest] = (where[longest] + shift) % values.shape[longest]
        spots.append(tuple(where))
    return values.at[spots[0]].set(least).at[spots[1]].set(high)


def cumulative_ranks(count, lean):
    loads = [(1 << 20) // math.isqrt(standing ** lean) + 1 for standing in range(1, count + 1)]
    width = 1 + sum(loads) // (1 << 30)
    return np.cumsum(np.array([max(1, weight // width) for weight in loads]))


def ranked(key, shape, number_of, skew):
    grid = cumulative_ranks(number_of, skew)
    ticket = jax.random.randint(jax.random.fold_in(key, 1), shape, 0, int(grid[number_of - 1]))
    standing = jnp.searchsorted(jnp.asarray(grid, jnp.int32), ticket, side="right")
    return jax.random.permutation(jax.random.fold_in(key, 2), number_of)[standing].astype(jnp.int32)


def setup_inputs(seed: int = 0) -> dict:
    key_of = jax.random.split(jax.random.key(seed), 4)
    hidden = draw_hidden(jax.random.fold_in(key_of[3], 71), 0)
    out_embed = draw_out_embed(jax.random.fold_in(key_of[3], 71), 0)
    labels = set_ends(ranked(key_of[2], (TOKENS,), VOCAB, 2), jax.random.fold_in(key_of[2], 3), 0, VOCAB - 1).astype(jnp.int32)
    return {"hidden": hidden, "out_embed": out_embed, "labels": labels}


def combine_stats(first, second):
    peak_first, mass_first, label_first = first
    peak_second, mass_second, label_second = second
    peak_value = jnp.maximum(peak_first, peak_second)
    exp_total = mass_first * jnp.exp(peak_first - peak_value) + mass_second * jnp.exp(peak_second - peak_value)
    return (peak_value, exp_total, label_first + label_second)


def reference(hidden, out_embed, labels):
    dense = hidden.astype(jnp.float32)
    row_block = math.gcd(VOCAB, 4096)
    block_total = VOCAB // row_block
    weight_blocks = out_embed.reshape(block_total, row_block, D)
    offsets = (jnp.arange(block_total) * row_block).astype(jnp.int32)

    def absorb(state_now, inputs):
        weight_block, offset = inputs
        logits = jnp.dot(dense, weight_block.astype(jnp.float32).T, precision=lax.Precision.HIGHEST)
        peak_block = jnp.max(logits, axis=1)
        mass_block = jnp.sum(jnp.exp(logits - peak_block[:, None]), axis=1)
        row_ids = offset + lax.broadcasted_iota(jnp.int32, logits.shape, 1)
        label_block = jnp.sum(jnp.where(row_ids == labels[:, None], logits, jnp.zeros_like(logits)), axis=1)
        return combine_stats(state_now, (peak_block, mass_block, label_block)), None

    initial = (jnp.full((TOKENS,), -1e30, jnp.float32), jnp.zeros((TOKENS,), jnp.float32), jnp.zeros((TOKENS,), jnp.float32))
    final_state, unused = lax.scan(absorb, initial, (weight_blocks, offsets))
    peak_value, exp_total, label_logit = final_state
    token_loss = jnp.log(exp_total) + peak_value - label_logit
    return token_loss, jnp.sum(token_loss) / TOKENS
```

```python
import functools

import jax
import jax.numpy as jnp
from jax import lax
from jax.experimental import pallas as pl
from jax.experimental.pallas import tpu as pltpu
from jax.sharding import Mesh
from jax.sharding import PartitionSpec as P

NX, NC, NZ, NY = 4, 2, 8, 4
ROWS = 128
PAIR = 2 * ROWS


class Message:
    def __init__(self, link, size, to, copy, deps):
        self.link, self.size, self.to, self.copy, self.deps = link, size, to, copy, deps
        self.index = None


def plan_messages(tokens, depth, vocab, width):
    m = {}
    blocks = vocab // ROWS
    pairs = blocks // 2
    xbytes = ROWS * width * 2
    for j in range(pairs):
        for d in (1, -1):
            order = (2 * j, 2 * j + 1) if d == 1 else (2 * j + 1, 2 * j)
            behind = []
            if j >= 2:
                behind = [("xo", d, 2 * (j - 2) + (1 if d == 1 else 0))]
            for b in order:
                m["xo", d, b] = Message(("x", d), xbytes, {"x": d}, ("own_e", 0, b * ROWS, ROWS), behind)
            b = order[0]
            m["xf", d, b] = Message(("x", d), xbytes, {"x": d}, ("e", -d, b * ROWS, ROWS), [("xo", d, b)])
        both = (2 * j, 2 * j + 1)
        for name, where, deps in (
            ("d1", -1, [("xo", 1, b) for b in both]),
            ("d2", 1, [("xo", -1, b) for b in both]),
            ("d3", 2, [("xf", 1, both[0]), ("xf", -1, both[1])]),
        ):
            m[name, j] = Message(("d",), 2 * xbytes, {"c": 1}, ("e", where, j * PAIR, PAIR), deps)
    m["do",] = Message(("d",), vocab * width * 2, {"c": 1}, ("own_e", 0, 0, vocab), [])

    half, quarter = tokens // 2, tokens // 4
    hbytes = half * depth * 2
    for d in (1, -1):
        for s in range(1, 5):
            at, n = (0, half) if s < 4 else ((0, quarter) if d == 1 else (quarter, quarter))
            kind = "own_h" if s == 1 else "h"
            deps = [] if s == 1 else [("az", d, s - 1)]
            m["az", d, s] = Message(("z", d), n * depth * 2, {"z": d}, (kind, (-d * (s - 1), 0), at, n), deps)
    for dz in range(-3, 5):
        if dz == 0:
            deps = []
        elif dz == 4:
            deps = [("az", 1, 4), ("az", -1, 4)]
        else:
            deps = [("az", 1, -dz)] if dz < 0 else [("az", -1, dz)]
        for d in (1, -1):
            m["ay", d, dz] = Message(("y", d), hbytes, {"y": d}, ("own_h" if dz == 0 else "h", (dz, 0), 0, half), deps)
        d = 1 if dz % 2 == 0 else -1
        m["ayf", d, dz] = Message(("y", d), hbytes, {"y": d}, ("h", (dz, -d), 0, half), [("ay", d, dz)])
    for d in (1, -1):
        m["by", d] = Message(("y", d), hbytes, {"y": d}, ("own_h", (0, 0), half, half), [])
        at = half if d == 1 else half + quarter
        m["byf", d] = Message(("y", d), hbytes // 2, {"y": d}, ("h", (0, -d), at, quarter), [("by", d)])
    for dy in (0, 1, -1, 2):
        first = {0: [], 1: [("by", -1)], -1: [("by", 1)], 2: [("byf", 1), ("byf", -1)]}[dy]
        for d in (1, -1):
            for s in range(1, 5):
                at, n = (half, half) if s < 4 else ((half, quarter) if d == 1 else (half + quarter, quarter))
                kind = "own_h" if s == 1 and dy == 0 else "h"
                deps = first if s == 1 else [("bz", d, dy, s - 1)]
                m["bz", d, dy, s] = Message(("z", d), n * depth * 2, {"z": d}, (kind, (-d * (s - 1), dy), at, n), deps)
    for i, one in enumerate(m.values()):
        one.index = i
    return m


def arrivals(m):
    rate = {"x": 46.0e3, "y": 46.0e3, "z": 46.0e3, "d": 500.0e3}
    free, when, left = {}, {}, dict(m)

    def send(name, now):
        one = m[name]
        begin = max(now, free.get(one.link, 0.0))
        free[one.link] = begin + one.size / rate[one.link[0]]
        when[name] = free[one.link] + (1.0 if one.link[0] == "d" else 2.0)
        del left[name]

    initial = [n for n in m if not m[n].deps]
    for n in initial:
        send(n, 0.0)
    order, done = [], set()
    while len(done) < len(m):
        n = min((k for k in when if k not in done), key=lambda k: (when[k], m[k].index))
        done.add(n)
        released = [k for k in left if all(q in done for q in m[k].deps)]
        for k in released:
            send(k, when[n])
        order.append((n, when[n], released))
    return initial, order


def program_order(m, pairs, step_us):
    initial, order = arrivals(m)
    hidden = {n for n in m if n[0] in ("az", "ay", "ayf", "by", "byf", "bz")}

    def needs(j):
        names = {("do",), ("d1", j), ("d2", j), ("d3", j)}
        for b in (2 * j, 2 * j + 1):
            names |= {("xo", 1, b), ("xo", -1, b)}
        names |= {("xf", 1, 2 * j), ("xf", -1, 2 * j + 1)}
        return names | hidden

    def early(j):
        return needs(j) - {("d3", j), ("xf", 1, 2 * j), ("xf", -1, 2 * j + 1)}

    out, waited, clock, i, j, part = [("send", initial)], set(), 0.0, 0, 0, 0
    while i < len(order) or j < pairs:
        idle = i == len(order) or order[i][1] > clock
        last = j == pairs - 1
        if j < pairs and idle and part == 0 and needs(j) <= waited:
            out.append(("matmul", j, 0, 4))
            clock += step_us
            j += 1
        elif last and idle and part == 0 and early(j) <= waited:
            out.append(("matmul", j, 0, 3))
            clock += step_us * 0.75
            part = 1
        elif last and idle and part == 1 and needs(j) <= waited:
            out.append(("matmul", j, 3, 4))
            j += 1
        else:
            n, t, released = order[i]
            clock = max(clock, t)
            out.append(("wait", n))
            waited.add(n)
            if released:
                out.append(("send", released))
            i += 1
    return out


def kernel(m, steps, total_tokens, hid, emb, lab, out, e, h, acc, top, mass, mark, sz, sy, sx, rows, sent, came, own, tail_sent, tail_came):
    x, c = lax.axis_index("x"), lax.axis_index("c")
    z, y = lax.axis_index("z"), lax.axis_index("y")
    size = {"x": NX, "c": NC, "z": NZ, "y": NY}
    pos = {"x": x, "c": c, "z": z, "y": y}
    tokens = lab.shape[1]
    vocab = emb.shape[0]

    def shifted(axis, d):
        return lax.rem(pos[axis] + (d + size[axis]), size[axis])

    def device(to):
        return {axis: shifted(axis, d) for axis, d in to.items()}

    barrier = pltpu.get_barrier_semaphore()
    peers = [{"z": d} for d in range(1, NZ)] + [{"y": d} for d in range(1, NY)]
    others = [{"x": dx, "c": dc} for dx in range(NX) for dc in range(NC) if dx or dc]
    for to in peers + others:
        pl.semaphore_signal(barrier, inc=1, device_id=device(to), device_id_type=pl.DeviceIdType.MESH)
    pl.semaphore_wait(barrier, len(peers) + len(others))

    def chunk_e(dx):
        return shifted("x", dx) * NC + c

    def chunk_h(dz, dy):
        return shifted("z", dz) * NY + shifted("y", dy)

    def descriptor(one):
        kind, where, at, n = one.copy
        part = pl.ds(at, n)
        if kind in ("own_e", "e"):
            dst = e.at[chunk_e(where), part]
            src = emb.at[part] if kind == "own_e" else dst
        else:
            dst = h.at[chunk_h(*where), part]
            src = hid.at[part] if kind == "own_h" else dst
        return pltpu.make_async_remote_copy(
            src_ref=src,
            dst_ref=dst,
            send_sem=sent.at[one.index],
            recv_sem=came.at[one.index],
            device_id=device(one.to),
            device_id_type=pl.DeviceIdType.MESH,
        )

    own_h = pltpu.make_async_copy(hid, h.at[chunk_h(0, 0)], own.at[0])
    own_e = pltpu.make_async_copy(emb, e.at[chunk_e(0)], own.at[1])

    top[...] = jnp.full_like(top, -1e30)
    mass[...] = jnp.zeros_like(mass)
    mark[...] = jnp.zeros_like(mark)

    first_row = (z * NY + y) * vocab

    def matmul(j, begin, end):
        part = pl.ds(j * PAIR, PAIR)

        def product(dx):
            at = lax.rem(x + dx, NX)
            left = jnp.concatenate([e[at * NC + i, part] for i in range(NC)], axis=1)
            each = left.shape[1] // hid.shape[1]
            right = jnp.concatenate([h[at * each + i] for i in range(each)], axis=1)
            return lax.dot_general(left, right, (((1,), (1,)), ((), ())), preferred_element_type=jnp.float32)

        if begin == 0:
            acc[...] = product(0)
            begin = 1

        def more(q, carry):
            acc[...] += product(lax.rem(q + 1, 3) + 1)
            return carry

        lax.fori_loop(begin, end, more, 0)

    def absorb(j):
        def lanes(t, carry):
            at = pl.ds(pl.multiple_of(t * 128, 128), 128)
            block = acc[:, at].reshape(PAIR // 8, 8, 128)
            before = top[:, at]
            peak = jnp.maximum(before, jnp.max(block, axis=0))
            mass[:, at] = mass[:, at] * jnp.exp(before - peak) + jnp.sum(jnp.exp(block - peak[None]), axis=0)
            top[:, at] = peak
            row = lax.broadcasted_iota(jnp.int32, block.shape, 0) * 8 + lax.broadcasted_iota(jnp.int32, block.shape, 1)
            wanted = jnp.broadcast_to(lab[:, at] - (first_row + j * PAIR), (8, 128))
            mark[:, at] += jnp.sum(jnp.where(row == wanted[None], block, 0.0), axis=0)
            return carry

        lax.fori_loop(0, tokens // 128, lanes, 0)

    started = False
    for step in steps:
        if step[0] == "send":
            for name in step[1]:
                descriptor(m[name]).start()
            if not started:
                own_h.start()
                own_e.start()
                started = True
        elif step[0] == "wait":
            descriptor(m[step[1]]).wait_recv()
        else:
            _, j, begin, end = step
            if j == 0:
                own_h.wait()
                own_e.wait()
            matmul(j, begin, end)
            if end == 4:
                absorb(j)

    peak = jnp.max(top[...], axis=0, keepdims=True)
    lse = peak + jnp.log(jnp.sum(mass[...] * jnp.exp(top[...] - peak), axis=0, keepdims=True))
    picked = jnp.sum(mark[...], axis=0, keepdims=True)
    sz[z] = jnp.zeros((16, 128), jnp.float32)
    for t in range(tokens // 128):
        sz[z, t : t + 1] = lse[:, t * 128 : (t + 1) * 128]
        sz[z, 8 + t : 9 + t] = picked[:, t * 128 : (t + 1) * 128]

    def exchange(buffer, at, targets, base):
        copies = [
            pltpu.make_async_remote_copy(
                src_ref=buffer.at[at],
                dst_ref=buffer.at[at],
                send_sem=tail_sent.at[base + i],
                recv_sem=tail_came.at[base + i],
                device_id=device(to),
                device_id_type=pl.DeviceIdType.MESH,
            )
            for i, to in enumerate(targets)
        ]
        for one in copies:
            one.start()
        for one in copies:
            one.wait_recv()
        return copies

    def joined(stats):
        lse, picked = stats[:, 0:8], stats[:, 8:16]
        peak = jnp.max(lse, axis=0)
        return peak + jnp.log(jnp.sum(jnp.exp(lse - peak[None]), axis=0)), jnp.sum(picked, axis=0)

    pending = exchange(sz, z, [{"z": d} for d in range(1, NZ)], 0)
    lse, picked = joined(sz[...])
    sy[y, 0:8] = lse
    sy[y, 8:16] = picked
    pending += exchange(sy, y, [{"y": d} for d in range(1, NY)], NZ - 1)
    lse, picked = joined(sy[...])
    real = lax.broadcasted_iota(jnp.int32, (8, 128), 0) < tokens // 128
    loss = jnp.where(real, lse - picked, 0.0)
    rows[...] = loss
    me = x * NC + c
    sx[me] = jnp.broadcast_to(jnp.sum(jnp.sum(loss, axis=0, keepdims=True), axis=1, keepdims=True), (8, 128))
    pending += exchange(sx, me, others, NZ - 1 + NY - 1)
    out[8:16] = jnp.sum(sx[...], axis=0) / total_tokens
    share = tokens // (NZ * NY)
    first = (z * NY + y) * share
    line, lane = first // 128, lax.rem(first, 128)
    two = jnp.concatenate([rows[pl.ds(line, 1)], rows[pl.ds(line + 1, 1)]], axis=1)
    two = jnp.broadcast_to(two, (8, 256))
    out[0:8] = pltpu.roll(two, lax.rem(256 - lane, 256), 1)[:, 0:128]

    for one in m.values():
        descriptor(one).wait_send()
    for one in pending:
        one.wait_send()


def body(hidden, out_embed, labels):
    tokens, depth = hidden.shape
    vocab, width = out_embed.shape
    m = plan_messages(tokens, depth, vocab, width)
    steps = program_order(m, vocab // PAIR, 2.5)
    total_tokens = tokens * NX * NC
    n_tail = NZ - 1 + NY - 1 + NX * NC - 1
    f32 = jnp.float32
    out = pl.pallas_call(
        functools.partial(kernel, m, steps, total_tokens),
        out_shape=jax.ShapeDtypeStruct((16, 128), f32),
        in_specs=[
            pl.BlockSpec(memory_space=pl.ANY),
            pl.BlockSpec(memory_space=pl.ANY),
            pl.BlockSpec(memory_space=pltpu.VMEM),
        ],
        out_specs=pl.BlockSpec(memory_space=pltpu.VMEM),
        scratch_shapes=[
            pltpu.VMEM((NX * NC, vocab, width), jnp.bfloat16),
            pltpu.VMEM((NZ * NY, tokens, depth), jnp.bfloat16),
            pltpu.VMEM((PAIR, tokens), f32),
            pltpu.VMEM((8, tokens), f32),
            pltpu.VMEM((8, tokens), f32),
            pltpu.VMEM((8, tokens), f32),
            pltpu.VMEM((NZ, 16, 128), f32),
            pltpu.VMEM((NY, 16, 128), f32),
            pltpu.VMEM((NX * NC, 8, 128), f32),
            pltpu.VMEM((8, 128), f32),
            pltpu.SemaphoreType.DMA((len(m),)),
            pltpu.SemaphoreType.DMA((len(m),)),
            pltpu.SemaphoreType.DMA((2,)),
            pltpu.SemaphoreType.DMA((n_tail,)),
            pltpu.SemaphoreType.DMA((n_tail,)),
        ],
        compiler_params=pltpu.CompilerParams(
            collective_id=0, has_side_effects=True, vmem_limit_bytes=60 * 1024 * 1024
        ),
    )(hidden, out_embed, labels.reshape(1, tokens))
    return out[0, : tokens // (NZ * NY)], out[8, 0]


def solution(mesh):
    finer = Mesh(mesh.devices.reshape(NX, NC, NZ, NY), ("x", "c", "z", "y"))
    dp, tensor = ("x", "c"), ("z", "y")
    return jax.shard_map(
        body,
        mesh=finer,
        in_specs=(P(dp, tensor), P(tensor, dp), P(dp)),
        out_specs=(P(dp + tensor), P()),
        check_vma=False,
    )
```

```python
import functools

import jax
import jax.numpy as jnp
from jax import lax
from jax.experimental import pallas as pl
from jax.experimental.pallas import tpu as pltpu
from jax.sharding import Mesh
from jax.sharding import PartitionSpec as P

NX, NC, NZ, NY = 4, 2, 8, 4
STEPS = (256,) * 7 + (192, 64)
TASKS = (
    ((0, 1), 0, 4),
    ((2, 3), 0, 4),
    ((4, 5), 0, 3),
    ((4,), 3, 4),
    ((5,), 3, 4),
    ((6,), 0, 3),
    ((7, 8), 0, 3),
    ((6,), 3, 4),
    ((7,), 3, 4),
    ((8,), 3, 4),
)
AHEAD, SPREAD = 2, 5
Z_FIRST = 448


class Message:
    def __init__(self, event, link, to, what, where, at, n, deps):
        self.event, self.link, self.to, self.deps = event, link, to, deps
        self.what, self.where, self.at, self.n = what, where, at, n


def plan_messages(tokens, depth, vocab, width):
    m = []
    early, late = {}, {}
    for i, (group, begin, end) in enumerate(TASKS):
        for j in group:
            if begin == 0:
                early[j] = i
            if end == 4:
                late[j] = i
    at = 0
    for j, step in enumerate(STEPS):
        n = step // 2
        behind = [("xo", min(j - AHEAD, SPREAD), 1)] if j >= AHEAD else []
        for d in (1, -1):
            mine, other = (at, at + n) if d == 1 else (at + n, at)
            m.append(Message(("xo", j, 0), ("x", d), {"x": d}, "e", 0, mine, n, behind))
            m.append(Message(("xo", j, 1), ("x", d), {"x": d}, "e", 0, other, n, behind))
            m.append(Message(("xf", j), ("x", d), {"x": d}, "e", -d, mine, n, [("xo", j, 0)]))
        for where in (-1, 1):
            m.append(Message(("d", early[j]), ("d",), {"c": 1}, "e", where, at, step, [("xo", j, 0), ("xo", j, 1)]))
        m.append(Message(("d", late[j]), ("d",), {"c": 1}, "e", 2, at, step, [("xf", j)]))
        at += step
    m.append(Message(("do",), ("d",), {"c": 1}, "e", 0, 0, vocab, [("xo", 1, 0)]))

    n = tokens - Z_FIRST
    for d in (1, -1):
        m.append(Message(("by",), ("y", d), {"y": d}, "h", (0, 0), Z_FIRST, n, []))
        at = Z_FIRST if d == 1 else Z_FIRST + n // 2
        m.append(Message(("byf",), ("y", d), {"y": d}, "h", (0, -d), at, n // 2, [("by",)]))

    def along_z(name, dy, at, n, first):
        for d in (1, -1):
            for s in range(1, 5):
                deps = first if s == 1 else [(name, dy, s - 1)]
                here, count = (at, n) if s < 4 else ((at, n // 2) if d == 1 else (at + n // 2, n // 2))
                m.append(Message((name, dy, s), ("z", d), {"z": d}, "h", (-d * (s - 1), dy), here, count, deps))

    along_z("az", 0, 0, Z_FIRST, [])
    for dz in (0, 1, -1, 2, -2, 3, -3, 4):
        deps = [("az", 0, abs(dz))] if dz else []
        for d in (1, -1):
            m.append(Message(("ay", dz), ("y", d), {"y": d}, "h", (dz, 0), 0, Z_FIRST, deps))
        d = 1 if dz % 2 == 0 else -1
        m.append(Message(("ayf", dz), ("y", d), {"y": d}, "h", (dz, -d), 0, Z_FIRST, [("ay", dz)]))
    for dy in (0, 1, -1, 2):
        along_z("bz", dy, Z_FIRST, tokens - Z_FIRST, {0: [], 1: [("by",)], -1: [("by",)], 2: [("byf",)]}[dy])
    for one in m:
        one.size = one.n * 2 * (width if one.what == "e" else depth)
    return m


def arrivals(m):
    rate = {"x": 46.5e3, "y": 46.5e3, "z": 46.5e3, "d": 500.0e3}
    free, when, left, count = {}, {}, list(m), {}
    for one in m:
        count[one.event] = count.get(one.event, 0) + 1

    def send(one, now):
        begin = max(now, free.get(one.link, 0.0))
        free[one.link] = begin + one.size / rate[one.link[0]]
        there = free[one.link] + (1.0 if one.link[0] == "d" else 2.0)
        when[one.event] = max(when.get(one.event, 0.0), there)
        count[one.event] -= 1

    initial = [one for one in m if not one.deps]
    for one in initial:
        send(one, 0.0)
    left = [one for one in m if one.deps]
    order, done = [], set()
    while any(k not in done for k in count):
        k = min((k for k in when if k not in done and not count[k]), key=lambda k: when[k])
        done.add(k)
        released = [one for one in left if done.issuperset(one.deps)]
        left = [one for one in left if one not in released]
        for one in released:
            send(one, when[k])
        order.append((k, when[k], released))
    return initial, order


def program_order(m, step_us):
    initial, order = arrivals(m)
    hidden = {one.event for one in m if one.what == "h"}

    def needs(i, task):
        group, begin, end = task
        names = {("d", i)}
        if begin == 0:
            names |= {("do",)} | {("xo", j, k) for j in group for k in (0, 1)}
        if end == 4:
            names |= {("xf", j) for j in group}
        return names | hidden

    todo = [(needs(i, task), task) for i, task in enumerate(TASKS)]
    out, waited, clock, i = [("send", initial)], set(), 0.0, 0
    while i < len(order) or todo:
        idle = i == len(order) or order[i][1] > clock
        if todo and idle and todo[0][0] <= waited:
            task = todo.pop(0)[1]
            out.append(("matmul", task))
            clock += step_us * sum(STEPS[j] for j in task[0]) * (task[2] - task[1]) / 1024
        else:
            k, t, released = order[i]
            clock = max(clock, t)
            out.append(("wait", k))
            waited.add(k)
            if released:
                out.append(("send", released))
            i += 1
    return out


def kernel(m, steps, hid, emb, lab, token_loss, mean_loss, e, h, acc, top, mass, mark, sz, s2, sl, rows, came, sent, own, tail_sent, tail_came):
    x, c = lax.axis_index("x"), lax.axis_index("c")
    z, y = lax.axis_index("z"), lax.axis_index("y")
    size = {"x": NX, "c": NC, "z": NZ, "y": NY}
    pos = {"x": x, "c": c, "z": z, "y": y}
    lines = lab.shape[0]
    tokens = lines * 128
    vocab = emb.shape[0]

    def shifted(axis, d):
        return lax.rem(pos[axis] + (d + size[axis]), size[axis])

    def device(to):
        return {axis: shifted(axis, d) for axis, d in to.items()}

    def chunk_e(dx):
        return shifted("x", dx) * NC + c

    def chunk_h(dz, dy):
        return shifted("z", dz) * NY + shifted("y", dy)

    own_e = pltpu.make_async_copy(emb, e.at[chunk_e(0)], own.at[0])
    own_h = pltpu.make_async_copy(hid, h.at[chunk_h(0, 0)], own.at[1])
    own_e.start()
    own_h.start()

    barrier = pltpu.get_barrier_semaphore()
    near = [{"x": 1}, {"x": -1}, {"c": 1}, {"z": 1}, {"z": -1}, {"y": 1}, {"y": -1}]
    for to in near:
        pl.semaphore_signal(barrier, inc=1, device_id=device(to), device_id_type=pl.DeviceIdType.MESH)
    top[...] = jnp.full_like(top, -1e30)
    mass[...] = jnp.zeros_like(mass)
    mark[...] = jnp.zeros_like(mark)
    own_e.wait()
    own_h.wait()
    pl.semaphore_wait(barrier, len(near))

    events = {}
    for one in m:
        events.setdefault(one.event, []).append(one)
    number = {event: i for i, event in enumerate(events)}

    def copy(src, dst, send_sem, recv_sem, to):
        return pltpu.make_async_remote_copy(
            src_ref=src,
            dst_ref=dst,
            send_sem=send_sem,
            recv_sem=recv_sem,
            device_id=device(to),
            device_id_type=pl.DeviceIdType.MESH,
        )

    def start_message(one):
        part = pl.ds(one.at, one.n)
        ref = e.at[chunk_e(one.where), part] if one.what == "e" else h.at[chunk_h(*one.where), part]
        copy(ref, ref, sent.at[0 if one.what == "e" else 1], came.at[number[one.event]], one.to).start()

    def wait_event(event):
        some = events[event]
        ref = e if some[0].what == "e" else h
        total = sum(one.n for one in some)
        chunks = next(k for k in range(1, 9) if total % k == 0 and total // k <= ref.shape[1])
        ref = ref.at[pl.ds(0, chunks), pl.ds(0, total // chunks)]
        copy(ref, ref, sent.at[0], came.at[number[event]], some[0].to).wait_recv()

    first_row = (z * NY + y) * vocab

    start = [sum(STEPS[:j]) for j in range(len(STEPS))]

    def matmul(first, n, begin, end):
        part = pl.ds(first, n)

        def product(dx):
            at = lax.rem(x + dx, NX)
            left = jnp.concatenate([e[at * NC + i, part] for i in range(NC)], axis=1)
            each = left.shape[1] // hid.shape[1]
            right = jnp.concatenate([h[at * each + i] for i in range(each)], axis=1)
            return lax.dot_general(left, right, (((1,), (1,)), ((), ())), preferred_element_type=jnp.float32)

        if begin == 0:
            acc[part] = product(0)
            begin = 1

        def more(q, carry):
            acc[part] += product(lax.rem(q + 1, 3) + 1)
            return carry

        lax.fori_loop(begin, end, more, 0)

    def absorb(first, n):
        def lanes(t, carry):
            at = pl.ds(pl.multiple_of(t * 128, 128), 128)
            block = acc[pl.ds(first, n), at].reshape(n // 8, 8, 128)
            before = top[:, at]
            peak = jnp.maximum(before, jnp.max(block, axis=0))
            mass[:, at] = mass[:, at] * jnp.exp(before - peak) + jnp.sum(jnp.exp(block - peak[None]), axis=0)
            top[:, at] = peak
            row = lax.broadcasted_iota(jnp.int32, block.shape, 0) * 8 + lax.broadcasted_iota(jnp.int32, block.shape, 1)
            wanted = jnp.broadcast_to(lab[pl.ds(t, 1)] - (first_row + first), (8, 128))
            mark[:, at] += jnp.sum(jnp.where(row == wanted[None], block, 0.0), axis=0)
            return carry

        lax.fori_loop(0, lines, lanes, 0)

    for step in steps:
        if step[0] == "send":
            for one in step[1]:
                start_message(one)
        elif step[0] == "wait":
            wait_event(step[1])
        else:
            group, begin, end = step[1]
            first, n = start[group[0]], sum(STEPS[j] for j in group)
            matmul(first, n, begin, end)
            if end == 4:
                absorb(first, n)

    peak = jnp.max(top[...], axis=0, keepdims=True)
    lse = peak + jnp.log(jnp.sum(mass[...] * jnp.exp(top[...] - peak), axis=0, keepdims=True))
    picked = jnp.sum(mark[...], axis=0, keepdims=True)
    for t in range(lines):
        sz[z, t : t + 1] = lse[:, t * 128 : (t + 1) * 128]
        sz[z, lines + t : lines + t + 1] = picked[:, t * 128 : (t + 1) * 128]

    def combined(lse, axis):
        peak = jnp.max(lse, axis=axis, keepdims=True)
        return jnp.squeeze(peak, axis) + jnp.log(jnp.sum(jnp.exp(lse - peak), axis=axis))

    def spread(i, buffer, at, targets):
        for to in targets:
            copy(buffer.at[at], buffer.at[at], tail_sent.at[i], tail_came.at[i], to).start()
        all_of_them = buffer.at[pl.ds(0, len(targets))]
        return copy(all_of_them, all_of_them, tail_sent.at[i], tail_came.at[i], targets[0])

    along_z = spread(0, sz, z, [{"z": d} for d in (4, 3, -3, 2, -2, 1, -1)])
    along_z.wait_recv()
    me = (x * NC + c) * NY + y
    picked = jnp.sum(sz[:, lines : 2 * lines], axis=0)
    s2[me, 0:lines] = combined(sz[:, 0:lines], 0)
    s2[me, lines : lines + 1] = jnp.sum(picked, axis=0, keepdims=True)
    sl[y] = picked
    order = (2, 1, -1, 0)
    across = spread(1, s2, me, [{"x": i, "y": j, "c": k} for i in order for j in order for k in (0, 1) if i or j or k])
    along_y = spread(2, sl, y, [{"y": j} for j in (2, 1, -1)])
    across.wait_recv()
    along_y.wait_recv()
    whole = s2[...].reshape(NX * NC, NY, lines + 1, 128)
    each = jnp.sum(combined(whole[:, :, 0:lines], 1), axis=1) - jnp.sum(whole[:, :, lines], axis=1)
    mean_loss[...] = jnp.sum(jnp.sum(each, axis=0, keepdims=True), axis=1, keepdims=True) / (tokens * NX * NC)
    mine = s2[pl.ds((x * NC + c) * NY, NY)]
    rows[0:lines] = combined(mine[:, 0:lines], 0) - jnp.sum(sl[...], axis=0)
    rows[lines : lines + 1] = jnp.zeros((1, 128), jnp.float32)
    share = tokens // (NZ * NY)
    first = (z * NY + y) * share
    line, lane = first // 128, lax.rem(first, 128)
    two = jnp.concatenate([rows[pl.ds(line, 1)], rows[pl.ds(line + 1, 1)]], axis=1)
    two = jnp.broadcast_to(two, (8, 256))
    token_loss[...] = pltpu.roll(two, lax.rem(256 - lane, 256), 1)[0:1, 0:share]

    for i, ref in enumerate((e, h)):
        one = [k for k in m if k.what == "eh"[i]]
        whole = ref.at[pl.ds(0, sum(k.n for k in one) // ref.shape[1])]
        copy(whole, whole, sent.at[i], came.at[0], one[0].to).wait_send()
    for one in (along_z, across, along_y):
        one.wait_send()


def body(hidden, out_embed, labels):
    tokens, depth = hidden.shape
    vocab, width = out_embed.shape
    lines = tokens // 128
    m = plan_messages(tokens, depth, vocab, width)
    steps = program_order(m, 2.4)
    f32 = jnp.float32
    token_loss, mean_loss = pl.pallas_call(
        functools.partial(kernel, m, steps),
        out_shape=(
            jax.ShapeDtypeStruct((1, tokens // (NZ * NY)), f32),
            jax.ShapeDtypeStruct((1, 1), f32),
        ),
        in_specs=[
            pl.BlockSpec(memory_space=pl.ANY),
            pl.BlockSpec(memory_space=pl.ANY),
            pl.BlockSpec(memory_space=pltpu.VMEM),
        ],
        out_specs=(pl.BlockSpec(memory_space=pltpu.VMEM), pl.BlockSpec(memory_space=pltpu.VMEM)),
        scratch_shapes=[
            pltpu.VMEM((NX * NC, vocab, width), jnp.bfloat16),
            pltpu.VMEM((NZ * NY, tokens, depth), jnp.bfloat16),
            pltpu.VMEM((vocab, tokens), f32),
            pltpu.VMEM((8, tokens), f32),
            pltpu.VMEM((8, tokens), f32),
            pltpu.VMEM((8, tokens), f32),
            pltpu.VMEM((NZ, 2 * lines, 128), f32),
            pltpu.VMEM((NX * NC * NY, lines + 1, 128), f32),
            pltpu.VMEM((NY, lines, 128), f32),
            pltpu.VMEM((lines + 1, 128), f32),
            pltpu.SemaphoreType.DMA((len({one.event for one in m}),)),
            pltpu.SemaphoreType.DMA((2,)),
            pltpu.SemaphoreType.DMA((2,)),
            pltpu.SemaphoreType.DMA((3,)),
            pltpu.SemaphoreType.DMA((3,)),
        ],
        compiler_params=pltpu.CompilerParams(
            collective_id=0, has_side_effects=True, vmem_limit_bytes=60 * 1024 * 1024
        ),
    )(hidden, out_embed, labels.reshape(lines, 128))
    return token_loss.reshape(-1), mean_loss.reshape(())


def solution(mesh):
    finer = Mesh(mesh.devices.reshape(NX, NC, NZ, NY), ("x", "c", "z", "y"))
    dp, tensor = ("x", "c"), ("z", "y")
    return jax.shard_map(
        body,
        mesh=finer,
        in_specs=(P(dp, tensor), P(tensor, dp), P(dp)),
        out_specs=(P(dp + tensor), P()),
        check_vma=False,
    )
```

```python
import functools

import jax
import jax.numpy as jnp
from jax import lax
from jax.experimental import pallas as pl
from jax.experimental.pallas import tpu as pltpu
from jax.sharding import Mesh
from jax.sharding import PartitionSpec as P

NX, NC, NZ, NY = 4, 2, 8, 4
STEPS = (256,) * 7 + (192, 64)
TASKS = (
    ((0, 1), 0, 4),
    ((2, 3), 0, 4),
    ((4, 5), 0, 3),
    ((4,), 3, 4),
    ((5,), 3, 4),
    ((6,), 0, 3),
    ((7, 8), 0, 3),
    ((6,), 3, 4),
    ((7, 8), 3, 3.5),
    ((7, 8), 3.5, 4),
)
AHEAD, SPREAD = 2, 5
Z_FIRST = 448


class Message:
    def __init__(self, event, link, to, what, where, at, n, deps):
        self.event, self.link, self.to, self.deps = event, link, to, deps
        self.what, self.where, self.at, self.n = what, where, at, n


def plan_messages(tokens, depth, vocab, width):
    m = []
    early, late = {}, {}
    for i, (group, begin, end) in enumerate(TASKS):
        for j in group:
            if begin == 0:
                early[j] = i
            if end == 4:
                late[j] = i
    at = 0
    for j, step in enumerate(STEPS):
        n = step // 2
        behind = [("xo", min(j - AHEAD, SPREAD), 1)] if j >= AHEAD else []
        for d in (1, -1):
            mine, other = (at, at + n) if d == 1 else (at + n, at)
            m.append(Message(("xo", j, 0), ("x", d), {"x": d}, "e", 0, mine, n, behind))
            m.append(Message(("xo", j, 1), ("x", d), {"x": d}, "e", 0, other, n, behind))
            m.append(Message(("xf", j), ("x", d), {"x": d}, "e", -d, mine, n, [("xo", j, 0)]))
        for where in (-1, 1):
            m.append(Message(("d", early[j]), ("d",), {"c": 1}, "e", where, at, step, [("xo", j, 0), ("xo", j, 1)]))
        m.append(Message(("d", late[j]), ("d",), {"c": 1}, "e", 2, at, step, [("xf", j)]))
        at += step
    m.append(Message(("do",), ("d",), {"c": 1}, "e", 0, 0, vocab, [("xo", 1, 0)]))

    n = tokens - Z_FIRST
    for d in (1, -1):
        m.append(Message(("by",), ("y", d), {"y": d}, "h", (0, 0), Z_FIRST, n, []))
        at = Z_FIRST if d == 1 else Z_FIRST + n // 2
        m.append(Message(("byf",), ("y", d), {"y": d}, "h", (0, -d), at, n // 2, [("by",)]))

    def along_z(name, dy, at, n, first):
        for d in (1, -1):
            for s in range(1, 5):
                deps = first if s == 1 else [(name, dy, s - 1)]
                here, count = (at, n) if s < 4 else ((at, n // 2) if d == 1 else (at + n // 2, n // 2))
                m.append(Message((name, dy, s), ("z", d), {"z": d}, "h", (-d * (s - 1), dy), here, count, deps))

    along_z("az", 0, 0, Z_FIRST, [])
    for dz in (0, 1, -1, 2, -2, 3, -3, 4):
        deps = [("az", 0, abs(dz))] if dz else []
        for d in (1, -1):
            m.append(Message(("ay", dz), ("y", d), {"y": d}, "h", (dz, 0), 0, Z_FIRST, deps))
        d = 1 if dz % 2 == 0 else -1
        m.append(Message(("ayf", dz), ("y", d), {"y": d}, "h", (dz, -d), 0, Z_FIRST, [("ay", dz)]))
    for dy in (0, 1, -1, 2):
        along_z("bz", dy, Z_FIRST, tokens - Z_FIRST, {0: [], 1: [("by",)], -1: [("by",)], 2: [("byf",)]}[dy])
    for one in m:
        one.size = one.n * 2 * (width if one.what == "e" else depth)
    return m


def arrivals(m):
    rate = {"x": 46.5e3, "y": 46.5e3, "z": 46.5e3, "d": 500.0e3}
    free, when, left, count = {}, {}, list(m), {}
    for one in m:
        count[one.event] = count.get(one.event, 0) + 1

    def send(one, now):
        begin = max(now, free.get(one.link, 0.0))
        free[one.link] = begin + one.size / rate[one.link[0]]
        there = free[one.link] + (1.0 if one.link[0] == "d" else 2.0)
        when[one.event] = max(when.get(one.event, 0.0), there)
        count[one.event] -= 1

    initial = [one for one in m if not one.deps]
    for one in initial:
        send(one, 0.0)
    left = [one for one in m if one.deps]
    order, done = [], set()
    while any(k not in done for k in count):
        k = min((k for k in when if k not in done and not count[k]), key=lambda k: when[k])
        done.add(k)
        released = [one for one in left if done.issuperset(one.deps)]
        left = [one for one in left if one not in released]
        for one in released:
            send(one, when[k])
        order.append((k, when[k], released))
    return initial, order


def program_order(m, step_us):
    initial, order = arrivals(m)
    hidden = {one.event for one in m if one.what == "h"}

    def needs(i, task):
        group, begin, end = task
        if end == 3.5:
            return {("xf", j) for j in group}
        names = {("d", i)}
        if begin == 0:
            names |= {("do",)} | {("xo", j, k) for j in group for k in (0, 1)}
        if end == 4:
            names |= {("xf", j) for j in group}
        return names | hidden

    todo = [(needs(i, task), task) for i, task in enumerate(TASKS)]
    out, waited, clock, i = [("send", initial)], set(), 0.0, 0
    while i < len(order) or todo:
        idle = i == len(order) or order[i][1] > clock
        if todo and idle and todo[0][0] <= waited:
            task = todo.pop(0)[1]
            out.append(("matmul", task))
            clock += step_us * sum(STEPS[j] for j in task[0]) * (task[2] - task[1]) / 1024
        else:
            k, t, released = order[i]
            clock = max(clock, t)
            out.append(("wait", k))
            waited.add(k)
            if released:
                out.append(("send", released))
            i += 1
    return out


def kernel(m, steps, hid, emb, lab_hbm, token_loss, mean_loss, lab, e, h, acc, top, mass, mark, sz, s2, lz, ly, rows, came, sent, own, tail_sent, tail_came):
    x, c = lax.axis_index("x"), lax.axis_index("c")
    z, y = lax.axis_index("z"), lax.axis_index("y")
    size = {"x": NX, "c": NC, "z": NZ, "y": NY}
    pos = {"x": x, "c": c, "z": z, "y": y}
    lines = lab_hbm.shape[0]
    tokens = lines * 128
    vocab = emb.shape[0]

    def shifted(axis, d):
        return lax.rem(pos[axis] + (d + size[axis]), size[axis])

    def device(to):
        return {axis: shifted(axis, d) for axis, d in to.items()}

    def chunk_e(dx):
        return shifted("x", dx) * NC + c

    def chunk_h(dz, dy):
        return shifted("z", dz) * NY + shifted("y", dy)

    first_rows = pl.ds(0, sum(STEPS[:AHEAD]))
    other_rows = pl.ds(sum(STEPS[:AHEAD]), vocab - sum(STEPS[:AHEAD]))
    own_first = pltpu.make_async_copy(emb.at[first_rows], e.at[chunk_e(0), first_rows], own.at[0])
    own_hidden = pltpu.make_async_copy(hid, h.at[chunk_h(0, 0)], own.at[1])
    own_other = pltpu.make_async_copy(emb.at[other_rows], e.at[chunk_e(0), other_rows], own.at[2])
    own_labels = pltpu.make_async_copy(lab_hbm, lab, own.at[3])
    own_first.start()

    barrier = pltpu.get_barrier_semaphore()
    near = [{"x": 1}, {"x": -1}, {"c": 1}, {"z": 1}, {"z": -1}, {"y": 1}, {"y": -1}]
    for to in near:
        pl.semaphore_signal(barrier, inc=1, device_id=device(to), device_id_type=pl.DeviceIdType.MESH)
    for one in (own_hidden, own_other, own_labels):
        one.start()
    top[...] = jnp.full_like(top, -1e30)
    mass[...] = jnp.zeros_like(mass)
    mark[...] = jnp.zeros_like(mark)
    own_first.wait()
    pl.semaphore_wait(barrier, len(near))

    events = {}
    for one in m:
        events.setdefault(one.event, []).append(one)
    number = {event: i for i, event in enumerate(events)}

    def copy(src, dst, send_sem, recv_sem, to):
        return pltpu.make_async_remote_copy(
            src_ref=src,
            dst_ref=dst,
            send_sem=send_sem,
            recv_sem=recv_sem,
            device_id=device(to),
            device_id_type=pl.DeviceIdType.MESH,
        )

    def start_message(one):
        part = pl.ds(one.at, one.n)
        ref = e.at[chunk_e(one.where), part] if one.what == "e" else h.at[chunk_h(*one.where), part]
        copy(ref, ref, sent.at[0 if one.what == "e" else 1], came.at[number[one.event]], one.to).start()

    def wait_event(event):
        some = events[event]
        ref = e if some[0].what == "e" else h
        total = sum(one.n for one in some)
        chunks = next(k for k in range(1, 9) if total % k == 0 and total // k <= ref.shape[1])
        ref = ref.at[pl.ds(0, chunks), pl.ds(0, total // chunks)]
        copy(ref, ref, sent.at[0], came.at[number[event]], some[0].to).wait_recv()

    first_row = (z * NY + y) * vocab

    start = [sum(STEPS[:j]) for j in range(len(STEPS))]

    def matmul(first, n, begin, end):
        part = pl.ds(first, n)

        def half(core):
            at = lax.rem(x + 2, NX) * NC + core
            each = emb.shape[1] // hid.shape[1]
            right = jnp.concatenate([h[at * each + i] for i in range(each)], axis=1)
            return lax.dot_general(e[at, part], right, (((1,), (1,)), ((), ())), preferred_element_type=jnp.float32)

        if begin == 3.5 or end == 3.5:
            acc[part] += half(c if end == 3.5 else 1 - c)
            return

        def product(dx):
            at = lax.rem(x + dx, NX)
            left = jnp.concatenate([e[at * NC + i, part] for i in range(NC)], axis=1)
            each = left.shape[1] // hid.shape[1]
            right = jnp.concatenate([h[at * each + i] for i in range(each)], axis=1)
            return lax.dot_general(left, right, (((1,), (1,)), ((), ())), preferred_element_type=jnp.float32)

        if begin == 0:
            acc[part] = product(0)
            begin = 1

        def more(q, carry):
            acc[part] += product(lax.rem(q + 1, 3) + 1)
            return carry

        lax.fori_loop(begin, end, more, 0)

    def absorb(first, n):
        def lanes(t, carry):
            at = pl.ds(pl.multiple_of(t * 128, 128), 128)
            block = acc[pl.ds(first, n), at].reshape(n // 8, 8, 128)
            before = top[:, at]
            peak = jnp.maximum(before, jnp.max(block, axis=0))
            mass[:, at] = mass[:, at] * jnp.exp(before - peak) + jnp.sum(jnp.exp(block - peak[None]), axis=0)
            top[:, at] = peak
            row = lax.broadcasted_iota(jnp.int32, block.shape, 0) * 8 + lax.broadcasted_iota(jnp.int32, block.shape, 1)
            wanted = jnp.broadcast_to(lab[pl.ds(t, 1)] - (first_row + first), (8, 128))
            mark[:, at] += jnp.sum(jnp.where(row == wanted[None], block, 0.0), axis=0)
            return carry

        lax.fori_loop(0, lines, lanes, 0)

    for step in steps:
        if step[0] == "send":
            if step[1][0].deps:
                for one in step[1]:
                    start_message(one)
                continue
            for one in step[1]:
                if one.what == "e":
                    start_message(one)
            own_hidden.wait()
            for one in step[1]:
                if one.what == "h":
                    start_message(one)
            for one in (own_other, own_labels):
                one.wait()
        elif step[0] == "wait":
            wait_event(step[1])
        else:
            group, begin, end = step[1]
            first, n = start[group[0]], sum(STEPS[j] for j in group)
            matmul(first, n, begin, end)
            if end == 4:
                absorb(first, n)

    peak = jnp.max(top[...], axis=0, keepdims=True)
    lse = peak + jnp.log(jnp.sum(mass[...] * jnp.exp(top[...] - peak), axis=0, keepdims=True))
    picked = jnp.sum(mark[...], axis=0, keepdims=True)
    for t in range(lines):
        sz[z, t : t + 1] = lse[:, t * 128 : (t + 1) * 128]
        lz[z, t : t + 1] = picked[:, t * 128 : (t + 1) * 128]
    sz[z, lines : lines + 1] = sum(picked[:, t * 128 : (t + 1) * 128] for t in range(lines))

    def combined(lse, axis):
        peak = jnp.max(lse, axis=axis, keepdims=True)
        return jnp.squeeze(peak, axis) + jnp.log(jnp.sum(jnp.exp(lse - peak), axis=axis))

    def spread(i, buffer, at, targets):
        for to in targets:
            copy(buffer.at[at], buffer.at[at], tail_sent.at[i], tail_came.at[i], to).start()
        all_of_them = buffer.at[pl.ds(0, len(targets))]
        return copy(all_of_them, all_of_them, tail_sent.at[i], tail_came.at[i], targets[0])

    ring = [{"z": d} for d in (4, 3, -3, 2, -2, 1, -1)]
    along_z = spread(0, sz, z, ring)
    labels_z = spread(1, lz, z, ring)
    along_z.wait_recv()
    me = (x * NC + c) * NY + y
    s2[me, 0:lines] = combined(sz[:, 0:lines], 0)
    s2[me, lines : lines + 1] = jnp.sum(sz[:, lines : lines + 1], axis=0)
    order = (2, 1, -1, 0)
    across = spread(2, s2, me, [{"x": i, "y": j, "c": k} for i in order for j in order for k in (0, 1) if i or j or k])
    labels_z.wait_recv()
    ly[y] = jnp.sum(lz[...], axis=0)
    labels_y = spread(3, ly, y, [{"y": j} for j in (2, 1, -1)])
    labels_y.wait_recv()
    across.wait_recv()
    whole = s2[...].reshape(NX * NC, NY, lines + 1, 128)
    each = jnp.sum(combined(whole[:, :, 0:lines], 1), axis=1) - jnp.sum(whole[:, :, lines], axis=1)
    mean_loss[...] = jnp.sum(jnp.sum(each, axis=0, keepdims=True), axis=1, keepdims=True) / (tokens * NX * NC)
    mine = s2[pl.ds((x * NC + c) * NY, NY)]
    rows[0:lines] = combined(mine[:, 0:lines], 0) - jnp.sum(ly[...], axis=0)
    rows[lines : lines + 1] = jnp.zeros((1, 128), jnp.float32)
    share = tokens // (NZ * NY)
    first = (z * NY + y) * share
    line, lane = first // 128, lax.rem(first, 128)
    two = jnp.concatenate([rows[pl.ds(line, 1)], rows[pl.ds(line + 1, 1)]], axis=1)
    two = jnp.broadcast_to(two, (8, 256))
    token_loss[...] = pltpu.roll(two, lax.rem(256 - lane, 256), 1)[0:1, 0:share]

    for i, ref in enumerate((e, h)):
        one = [k for k in m if k.what == "eh"[i]]
        whole = ref.at[pl.ds(0, sum(k.n for k in one) // ref.shape[1])]
        copy(whole, whole, sent.at[i], came.at[0], one[0].to).wait_send()
    for one in (along_z, labels_z, across, labels_y):
        one.wait_send()


def body(hidden, out_embed, labels):
    tokens, depth = hidden.shape
    vocab, width = out_embed.shape
    lines = tokens // 128
    m = plan_messages(tokens, depth, vocab, width)
    steps = program_order(m, 2.4)
    f32 = jnp.float32
    token_loss, mean_loss = pl.pallas_call(
        functools.partial(kernel, m, steps),
        out_shape=(
            jax.ShapeDtypeStruct((1, tokens // (NZ * NY)), f32),
            jax.ShapeDtypeStruct((1, 1), f32),
        ),
        in_specs=[
            pl.BlockSpec(memory_space=pl.ANY),
            pl.BlockSpec(memory_space=pl.ANY),
            pl.BlockSpec(memory_space=pl.ANY),
        ],
        out_specs=(pl.BlockSpec(memory_space=pltpu.VMEM), pl.BlockSpec(memory_space=pltpu.VMEM)),
        scratch_shapes=[
            pltpu.VMEM((lines, 128), jnp.int32),
            pltpu.VMEM((NX * NC, vocab, width), jnp.bfloat16),
            pltpu.VMEM((NZ * NY, tokens, depth), jnp.bfloat16),
            pltpu.VMEM((vocab, tokens), f32),
            pltpu.VMEM((8, tokens), f32),
            pltpu.VMEM((8, tokens), f32),
            pltpu.VMEM((8, tokens), f32),
            pltpu.VMEM((NZ, lines + 1, 128), f32),
            pltpu.VMEM((NX * NC * NY, lines + 1, 128), f32),
            pltpu.VMEM((NZ, lines, 128), f32),
            pltpu.VMEM((NY, lines, 128), f32),
            pltpu.VMEM((lines + 1, 128), f32),
            pltpu.SemaphoreType.DMA((len({one.event for one in m}),)),
            pltpu.SemaphoreType.DMA((2,)),
            pltpu.SemaphoreType.DMA((4,)),
            pltpu.SemaphoreType.DMA((4,)),
            pltpu.SemaphoreType.DMA((4,)),
        ],
        compiler_params=pltpu.CompilerParams(
            collective_id=0, has_side_effects=True, vmem_limit_bytes=60 * 1024 * 1024
        ),
    )(hidden, out_embed, labels.reshape(lines, 128))
    return token_loss.reshape(-1), mean_loss.reshape(())


def solution(mesh):
    finer = Mesh(mesh.devices.reshape(NX, NC, NZ, NY), ("x", "c", "z", "y"))
    dp, tensor = ("x", "c"), ("z", "y")
    return jax.shard_map(
        body,
        mesh=finer,
        in_specs=(P(dp, tensor), P(tensor, dp), P(dp)),
        out_specs=(P(dp + tensor), P()),
        check_vma=False,
    )
```

```python
import functools

import jax
import jax.numpy as jnp
from jax import lax
from jax.experimental import pallas as pl
from jax.experimental.pallas import tpu as pltpu
from jax.sharding import Mesh
from jax.sharding import PartitionSpec as P

NX, NC, NZ, NY = 4, 2, 8, 4
BLOCKS = 4
OWN_Z, PART_Z = 480, 320
VIA_P = 192
TILE = 512
SLOW = {
    "o": {
        ("bz", 0): [("az", "o", 0, 2)],
        ("bz", 1): [("az", "o", 0, 2)],
        ("bz", 2): [("az", "o", 0, 1)],
    },
    "p": {
        "az": [("az", "o", 0, 4)],
        "ay": [("ay", "o", 4)],
        ("bz", 0): [("bz", "o", 0, 3)],
        ("bz", 1): [("bz", "o", 1, 3)],
        ("bz", -1): [("bz", "o", 2, 4)],
        ("bz", 2): [("bz", "o", 2, 4)],
    },
}
ROLES = ("me", "p", "q", "opp")


class Message:
    def __init__(self, event, link, to, what, where, at, n, deps, group):
        self.event, self.link, self.to, self.deps = event, link, to, deps
        self.what, self.where, self.at, self.n, self.group = what, where, at, n, group


def plan_messages(tokens, depth, vocab, width):
    m = []
    rows = vocab // 2
    step = rows // BLOCKS
    kept = tokens - VIA_P

    def add(event, link, to, what, where, at, n, deps, group):
        m.append(Message(event, link, to, what, where, at, n, deps, group))

    def gather(t, base, n_z, n_y, first, slow, group):
        def send(name, d_axis, d, where, at, n, deps):
            add(name, (d_axis, d), {d_axis: d}, "h", where, at, n, deps, group)

        at_y = base + n_z
        for d in (1, -1):
            send(("by", t), "y", d, (0, 0), at_y, n_y, first)
            send(("byf", t), "y", d, (0, -d), at_y if d == 1 else at_y + n_y // 2, n_y // 2, [("by", t)])

        def along_z(name, dy, at, n, before):
            for d in (1, -1):
                for s in range(1, 5):
                    deps = before if s == 1 else [(name, t, dy, s - 1)]
                    here, count = (at, n) if s < 4 else ((at, n // 2) if d == 1 else (at + n // 2, n // 2))
                    send((name, t, dy, s), "z", d, (-d * (s - 1), dy), here, count, deps)

        along_z("az", 0, base, n_z, first + slow.get("az", []))
        for dz in (0, 1, -1, 2, -2, 3, -3, 4):
            deps = [("az", t, 0, abs(dz))] if dz else first + slow.get("ay", [])
            for d in (1, -1):
                send(("ay", t, dz), "y", d, (dz, 0), base, n_z, deps)
            d = 1 if dz % 2 == 0 else -1
            send(("ayf", t, dz), "y", d, (dz, -d), base, n_z, [("ay", t, dz)])
        for dy in (0, 1, -1, 2):
            before = {0: first, 1: [("by", t)], -1: [("by", t)], 2: [("byf", t)]}[dy]
            along_z("bz", dy, at_y, n_y, before + slow.get(("bz", dy), []))

    add(("ph",), ("p",), {"p": 1}, "ht", (0, 0), 0, kept, [], 2)
    add(("lab",), ("p",), {"p": 1}, "lab", 0, 0, 0, [], 3)
    for j in range(BLOCKS):
        add(("e1", j), ("q",), {"q": 1}, "e", "me", j * step, step, [], 0)
        last = [("by", "o"), ("byf", "o")] if j == BLOCKS - 1 else []
        add(("e2", j), ("p",), {"p": 1}, "eo", "me", j * step, step, last, 0)
        add(("e3", j), ("q",), {"q": 1}, "e", "p", j * step, step, [("e2", j)], 0)
        for role, name in (("q", "e1"), ("p", "e2"), ("opp", "e3")):
            add(("d", role), ("d",), {"c": 1}, "e", role, j * step, step, [(name, j)], 0)
    add(("d", "me"), ("d",), {"c": 1}, "e", "me", 0, rows, [("by", "o")], 0)
    gather("o", 0, OWN_Z, tokens - OWN_Z, [], SLOW["o"], 1)
    for dz in (0, 1, -1, 2, -2, 3, -3, 4):
        for dy in (0, 1, -1, 2):
            deps = {0: [], 1: [("by", "o")], -1: [("by", "o")], 2: [("byf", "o")]}[dy] if dz == 0 else [("bz", "o", dy, abs(dz))]
            add(("pp", abs(dz)), ("p",), {"p": 1}, "ht", (dz, dy), kept, VIA_P, deps, 2)
    gather("p", tokens, PART_Z, kept - PART_Z, [("ph",)], SLOW["p"], 2)
    for one in m:
        one.size = one.n * 2 * (width if one.what in ("e", "eo") else depth)
    return m


def arrivals(m):
    rate = {"p": 46.0e3, "q": 46.0e3, "y": 46.0e3, "z": 46.0e3, "d": 500.0e3}
    free, when, count = {}, {}, {}
    for one in m:
        count[one.event] = count.get(one.event, 0) + 1

    def send(one, now):
        begin = max(now, free.get(one.link, 0.0))
        free[one.link] = begin + one.size / rate[one.link[0]]
        there = free[one.link] + (1.0 if one.link[0] == "d" else 2.0)
        when[one.event] = max(when.get(one.event, 0.0), there)
        count[one.event] -= 1

    initial = [one for one in m if not one.deps]
    for one in initial:
        send(one, 0.0)
    left = [one for one in m if one.deps]
    order, done = [], set()
    while any(k not in done for k in count):
        k = min((k for k in when if k not in done and not count[k]), key=lambda k: when[k])
        done.add(k)
        released = [one for one in left if done.issuperset(one.deps)]
        left = [one for one in left if one not in released]
        for one in released:
            send(one, when[k])
        order.append((k, when[k], released))
    return initial, order


def program_order(m):
    initial, order = arrivals(m)
    events = {one.event for one in m}
    embed = {"me": {("d", "me")}}
    for role, name in (("q", "e1"), ("p", "e2"), ("opp", "e3")):
        embed[role] = {("d", role)} | {k for k in events if k[0] == name}
    own = {k for k in events if len(k) > 1 and k[1] == "o"}
    todo = [(own | embed[role] | {("lab",)}, (role, 0), 3.4 if role == "opp" else 2.2) for role in ROLES]
    for d in range(5):
        mine = {("pp", d)}
        for k in events:
            if len(k) > 1 and k[1] == "p" and k[0] != "d" and (abs(k[-1]) if k[0] not in ("by", "byf") else 0) == d:
                mine.add(k)
        if d == 0:
            mine.add(("ph",))
        todo.append((mine, (d, 1), 1.1 if d in (0, 4) else 2.2))
    out, waited, clock, i = [("send", initial)], set(), 0.0, 0
    while i < len(order) or todo:
        idle = i == len(order) or order[i][1] > clock
        if todo and idle and todo[0][0] <= waited:
            _, task, cost = todo.pop(0)
            out.append(("matmul", task))
            clock += cost
        else:
            k, t, released = order[i]
            clock = max(clock, t)
            out.append(("wait", k))
            waited.add(k)
            if released:
                out.append(("send", released))
            i += 1
    return out


def kernel(m, steps, hid, emb, lab_hbm, token_loss, mean_loss, lab, e, eo, h, acc, top, mass, mark, sz, sp, s2, lz, lp, ly, rows, came, sent, own, tail_sent, tail_came):
    x, c = lax.axis_index("x"), lax.axis_index("c")
    z, y = lax.axis_index("z"), lax.axis_index("y")
    size = {"x": NX, "c": NC, "z": NZ, "y": NY}
    pos = {"x": x, "c": c, "z": z, "y": y}
    lines = lab_hbm.shape[0]
    tokens = lines * 128
    vocab = emb.shape[0]
    half = vocab // 2
    sign = 1 - 2 * lax.rem(x, 2)
    chip = {"me": x, "p": x + sign, "q": lax.rem(x - sign + NX, NX), "opp": lax.rem(x + 2, NX)}
    mine = lax.rem((x + 1) // 2, 2) * half
    other = half - mine

    def shifted(axis, d):
        return lax.rem(pos[axis] + (d + size[axis]), size[axis])

    def device(to):
        where = {axis: shifted(axis, d) for axis, d in to.items() if axis not in ("p", "q")}
        for role in ("p", "q"):
            if role in to:
                where["x"] = chip[role]
        return where

    def chunk_e(role):
        return chip[role] * NC + c

    def chunk_h(dz, dy):
        return shifted("z", dz) * NY + shifted("y", dy)

    own_eo = pltpu.make_async_copy(emb.at[pl.ds(pl.multiple_of(other, half), half)], eo, own.at[0])
    own_e = pltpu.make_async_copy(emb.at[pl.ds(pl.multiple_of(mine, half), half)], e.at[chunk_e("me")], own.at[1])
    own_h = pltpu.make_async_copy(hid, h.at[chunk_h(0, 0), pl.ds(0, tokens)], own.at[2])
    own_labels = pltpu.make_async_copy(lab_hbm, lab.at[0], own.at[3])
    loads = (own_h, own_labels, own_e, own_eo)
    own_h.start()

    barrier = pltpu.get_barrier_semaphore()
    near = [{"x": 1}, {"x": -1}, {"c": 1}, {"z": 1}, {"z": -1}, {"y": 1}, {"y": -1}]
    for to in near:
        pl.semaphore_signal(barrier, inc=1, device_id=device(to), device_id_type=pl.DeviceIdType.MESH)
    for one in loads[1:]:
        one.start()
    top[...] = jnp.full_like(top, -1e30)
    mass[...] = jnp.zeros_like(mass)
    mark[...] = jnp.zeros_like(mark)
    for one in loads:
        one.wait()
    pl.semaphore_wait(barrier, len(near))

    events = {}
    for one in m:
        events.setdefault(one.event, []).append(one)
    number = {event: i for i, event in enumerate(events)}

    def copy(src, dst, send_sem, recv_sem, to):
        return pltpu.make_async_remote_copy(
            src_ref=src,
            dst_ref=dst,
            send_sem=send_sem,
            recv_sem=recv_sem,
            device_id=device(to),
            device_id_type=pl.DeviceIdType.MESH,
        )

    def start_message(one):
        part = pl.ds(one.at, one.n)
        if one.what == "e":
            src = dst = e.at[chunk_e(one.where), part]
        elif one.what == "eo":
            src, dst = eo.at[part], e.at[chunk_e("me"), part]
        elif one.what == "h":
            src = dst = h.at[chunk_h(*one.where), part]
        elif one.what == "ht":
            src, dst = h.at[chunk_h(*one.where), part], h.at[chunk_h(*one.where), pl.ds(tokens + one.at, one.n)]
        else:
            src, dst = lab.at[0], lab.at[1]
        copy(src, dst, sent.at[one.group], came.at[number[one.event]], one.to).start()

    def wait_event(event):
        some = events[event]
        if some[0].what == "lab":
            ref = lab.at[1]
        else:
            ref = e if some[0].what in ("e", "eo") else h
            total = sum(one.n for one in some)
            chunks = next(k for k in range(1, 9) if total % (16 * k) == 0 and total // k <= ref.shape[1])
            ref = ref.at[pl.ds(0, chunks), pl.ds(0, total // chunks)]
        copy(ref, ref, sent.at[0], came.at[number[event]], some[0].to).wait_recv()

    first_row = (z * NY + y) * vocab + mine

    def matmul(part, token_set):
        at = pl.ds(token_set * tokens, tokens)
        if part in ROLES:
            chunks = [chip[part] * NC + i for i in range(NC)]
        else:
            chunks = [shifted("z", d) for d in sorted({part, part if part in (0, 4) else -part})]
        each = emb.shape[1] // hid.shape[1]

        def tile(i, carry):
            to = pl.ds(pl.multiple_of(i * TILE, TILE), TILE)
            left = jnp.concatenate([e[f, to] for f in chunks], axis=1)
            right = jnp.concatenate([h[f * each + i, at] for f in chunks for i in range(each)], axis=1)
            acc[to, at] += lax.dot_general(left, right, (((1,), (1,)), ((), ())), preferred_element_type=jnp.float32)
            return carry

        lax.fori_loop(0, half // TILE, tile, 0)

    def absorb(token_set):
        n = 256

        def lanes(t, carry):
            at = pl.ds(pl.multiple_of(token_set * tokens + lax.rem(t, lines) * 128, 128), 128)
            first = pl.multiple_of(t // lines * n, n)
            block = acc[pl.ds(first, n), at].reshape(n // 8, 8, 128)
            before = top[:, at]
            peak = jnp.maximum(before, jnp.max(block, axis=0))
            mass[:, at] = mass[:, at] * jnp.exp(before - peak) + jnp.sum(jnp.exp(block - peak[None]), axis=0)
            top[:, at] = peak
            row = lax.broadcasted_iota(jnp.int32, block.shape, 0) * 8 + lax.broadcasted_iota(jnp.int32, block.shape, 1)
            wanted = jnp.broadcast_to(lab[token_set, pl.ds(lax.rem(t, lines), 1)] - (first_row + first), (8, 128))
            mark[:, at] += jnp.sum(jnp.where(row == wanted[None], block, 0.0), axis=0)
            return carry

        lax.fori_loop(0, lines * (half // n), lanes, 0)

    for step in steps:
        if step[0] == "send":
            for one in step[1]:
                start_message(one)
            if not step[1][0].deps:

                def clear(i, carry):
                    acc[pl.ds(pl.multiple_of(i * 16, 16), 16)] = jnp.zeros((16, 2 * tokens), jnp.float32)
                    return carry

                lax.fori_loop(0, half // 16, clear, 0)
        elif step[0] == "wait":
            wait_event(step[1])
        else:
            matmul(*step[1])
            if step[1][0] in ("opp", 4):
                absorb(step[1][1])

    peak = jnp.max(top[...], axis=0, keepdims=True)
    lse = peak + jnp.log(jnp.sum(mass[...] * jnp.exp(top[...] - peak), axis=0, keepdims=True))
    picked = jnp.sum(mark[...], axis=0, keepdims=True)
    slot = 2 * z
    for token_set, (to_s, to_l) in enumerate(((sz.at[slot], lz.at[slot]), (sp, lp))):
        one = [slice(token_set * tokens + t * 128, token_set * tokens + (t + 1) * 128) for t in range(lines)]
        for t in range(lines):
            to_s[t : t + 1] = lse[:, one[t]]
            to_l[t : t + 1] = picked[:, one[t]]
        to_s[lines : lines + 1] = sum(picked[:, k] for k in one)

    def combined(lse, axis):
        peak = jnp.max(lse, axis=axis, keepdims=True)
        return jnp.squeeze(peak, axis) + jnp.log(jnp.sum(jnp.exp(lse - peak), axis=axis))

    def spread(i, buffer, work):
        for src, at, to in work:
            copy(src, buffer.at[at], tail_sent.at[i], tail_came.at[i], to).start()
        all_of_them = buffer.at[pl.ds(0, len(work))]
        return copy(all_of_them, all_of_them, tail_sent.at[i], tail_came.at[i], work[0][2])

    ring = (4, 3, -3, 2, -2, 1, -1, 0)

    def along(buffer, part):
        return [w for d in ring for w in ((part, slot + 1, {"p": 1, "z": d}), (buffer.at[slot], slot, {"z": d}))][:-1]

    along_z = spread(0, sz, along(sz, sp))
    labels_z = spread(1, lz, along(lz, lp))
    along_z.wait_recv()
    me = (x * NC + c) * NY + y
    s2[me, 0:lines] = combined(sz[:, 0:lines], 0)
    s2[me, lines : lines + 1] = jnp.sum(sz[:, lines : lines + 1], axis=0)
    order = (2, 1, -1, 0)
    across = spread(2, s2, [(s2.at[me], me, {"x": i, "y": j, "c": k}) for i in order for j in order for k in (0, 1) if i or j or k])
    labels_z.wait_recv()
    ly[y] = jnp.sum(lz[...], axis=0)
    labels_y = spread(3, ly, [(ly.at[y], y, {"y": j}) for j in (2, 1, -1)])
    labels_y.wait_recv()
    across.wait_recv()
    whole = s2[...].reshape(NX * NC, NY, lines + 1, 128)
    each = jnp.sum(combined(whole[:, :, 0:lines], 1), axis=1) - jnp.sum(whole[:, :, lines], axis=1)
    mean_loss[...] = jnp.sum(jnp.sum(each, axis=0, keepdims=True), axis=1, keepdims=True) / (tokens * NX * NC)
    group = s2[pl.ds((x * NC + c) * NY, NY)]
    rows[0:lines] = combined(group[:, 0:lines], 0) - jnp.sum(ly[...], axis=0)
    rows[lines : lines + 1] = jnp.zeros((1, 128), jnp.float32)
    share = tokens // (NZ * NY)
    first = (z * NY + y) * share
    line, lane = first // 128, lax.rem(first, 128)
    two = jnp.concatenate([rows[pl.ds(line, 1)], rows[pl.ds(line + 1, 1)]], axis=1)
    two = jnp.broadcast_to(two, (8, 256))
    token_loss[...] = pltpu.roll(two, lax.rem(256 - lane, 256), 1)[0:1, 0:share]

    for group in range(4):
        some = [one for one in m if one.group == group]
        if group == 3:
            ref = lab.at[0]
        else:
            ref, n = (e, half) if group == 0 else (h, tokens)
            ref = ref.at[pl.ds(0, sum(one.n for one in some) // n), pl.ds(0, n)]
        copy(ref, ref, sent.at[group], came.at[0], some[0].to).wait_send()
    for one in (along_z, labels_z, across, labels_y):
        one.wait_send()


def body(hidden, out_embed, labels):
    tokens, depth = hidden.shape
    vocab, width = out_embed.shape
    lines = tokens // 128
    m = plan_messages(tokens, depth, vocab, width)
    steps = program_order(m)
    f32 = jnp.float32
    token_loss, mean_loss = pl.pallas_call(
        functools.partial(kernel, m, steps),
        out_shape=(
            jax.ShapeDtypeStruct((1, tokens // (NZ * NY)), f32),
            jax.ShapeDtypeStruct((1, 1), f32),
        ),
        in_specs=[
            pl.BlockSpec(memory_space=pl.ANY),
            pl.BlockSpec(memory_space=pl.ANY),
            pl.BlockSpec(memory_space=pl.ANY),
        ],
        out_specs=(pl.BlockSpec(memory_space=pltpu.VMEM), pl.BlockSpec(memory_space=pltpu.VMEM)),
        scratch_shapes=[
            pltpu.VMEM((2, lines, 128), jnp.int32),
            pltpu.VMEM((NX * NC, vocab // 2, width), jnp.bfloat16),
            pltpu.VMEM((vocab // 2, width), jnp.bfloat16),
            pltpu.VMEM((NZ * NY, 2 * tokens, depth), jnp.bfloat16),
            pltpu.VMEM((vocab // 2, 2 * tokens), f32),
            pltpu.VMEM((8, 2 * tokens), f32),
            pltpu.VMEM((8, 2 * tokens), f32),
            pltpu.VMEM((8, 2 * tokens), f32),
            pltpu.VMEM((2 * NZ, lines + 1, 128), f32),
            pltpu.VMEM((lines + 1, 128), f32),
            pltpu.VMEM((NX * NC * NY, lines + 1, 128), f32),
            pltpu.VMEM((2 * NZ, lines, 128), f32),
            pltpu.VMEM((lines, 128), f32),
            pltpu.VMEM((NY, lines, 128), f32),
            pltpu.VMEM((lines + 1, 128), f32),
            pltpu.SemaphoreType.DMA((len({one.event for one in m}),)),
            pltpu.SemaphoreType.DMA((4,)),
            pltpu.SemaphoreType.DMA((4,)),
            pltpu.SemaphoreType.DMA((4,)),
            pltpu.SemaphoreType.DMA((4,)),
        ],
        compiler_params=pltpu.CompilerParams(
            collective_id=0, has_side_effects=True, vmem_limit_bytes=60 * 1024 * 1024
        ),
    )(hidden, out_embed, labels.reshape(lines, 128))
    return token_loss.reshape(-1), mean_loss.reshape(())


def solution(mesh):
    finer = Mesh(mesh.devices.reshape(NX, NC, NZ, NY), ("x", "c", "z", "y"))
    dp, tensor = ("x", "c"), ("z", "y")
    return jax.shard_map(
        body,
        mesh=finer,
        in_specs=(P(dp, tensor), P(tensor, dp), P(dp)),
        out_specs=(P(dp + tensor), P()),
        check_vma=False,
    )
```

```python
import functools

import jax
import jax.numpy as jnp
from jax import lax
from jax.experimental import pallas as pl
from jax.experimental.pallas import tpu as pltpu
from jax.sharding import Mesh
from jax.sharding import PartitionSpec as P

NX, NC, NZ, NY = 4, 2, 8, 4
BLOCKS = 4
OWN_Z, PART_Z = 480, 320
SOONER = 2.5
VIA_P = 192
TILE = 512
ABSORB_AT = 7
SLOW = {
    "o": {
        ("bz", 0): [("az", "o", 0, 2)],
        ("bz", 1): [("az", "o", 0, 2)],
        ("bz", 2): [("az", "o", 0, 1)],
    },
    "p": {
        "az": [("az", "o", 0, 4)],
        "ay": [("ay", "o", 4)],
        ("bz", 0): [("bz", "o", 0, 3)],
        ("bz", 1): [("bz", "o", 1, 3)],
        ("bz", -1): [("bz", "o", 2, 4)],
        ("bz", 2): [("bz", "o", 2, 4)],
    },
}
ROLES = ("me", "p", "q", "opp")


class Message:
    def __init__(self, event, link, to, what, where, at, n, deps, group):
        self.event, self.link, self.to, self.deps = event, link, to, deps
        self.what, self.where, self.at, self.n, self.group = what, where, at, n, group


def plan_messages(tokens, depth, vocab, width):
    m = []
    rows = vocab // 2
    step = rows // BLOCKS
    kept = tokens - VIA_P

    def add(event, link, to, what, where, at, n, deps, group):
        m.append(Message(event, link, to, what, where, at, n, deps, group))

    def gather(t, base, n_z, n_y, first, slow, group):
        def send(name, d_axis, d, where, at, n, deps):
            add(name, (d_axis, d), {d_axis: d}, "h", where, at, n, deps, group)

        at_y = base + n_z
        for d in (1, -1):
            send(("by", t), "y", d, (0, 0), at_y, n_y, first)
            send(("byf", t), "y", d, (0, -d), at_y if d == 1 else at_y + n_y // 2, n_y // 2, [("by", t)])

        def along_z(name, dy, at, n, before):
            for d in (1, -1):
                for s in range(1, 5):
                    deps = before if s == 1 else [(name, t, dy, s - 1)]
                    here, count = (at, n) if s < 4 else ((at, n // 2) if d == 1 else (at + n // 2, n // 2))
                    send((name, t, dy, s), "z", d, (-d * (s - 1), dy), here, count, deps)

        along_z("az", 0, base, n_z, first + slow.get("az", []))
        for dz in (0, 1, -1, 2, -2, 3, -3, 4):
            deps = [("az", t, 0, abs(dz))] if dz else first + slow.get("ay", [])
            for d in (1, -1):
                send(("ay", t, dz), "y", d, (dz, 0), base, n_z, deps)
            d = 1 if dz % 2 == 0 else -1
            send(("ayf", t, dz), "y", d, (dz, -d), base, n_z, [("ay", t, dz)])
        for dy in (0, 1, -1, 2):
            before = {0: first, 1: [("by", t)], -1: [("by", t)], 2: [("byf", t)]}[dy]
            along_z("bz", dy, at_y, n_y, before + slow.get(("bz", dy), []))

    add(("ph",), ("p",), {"p": 1}, "ht", (0, 0), 0, kept, [], 2)
    add(("lab",), ("p",), {"p": 1}, "lab", 0, 0, 0, [], 3)
    for j in range(BLOCKS):
        add(("e1", j), ("q",), {"q": 1}, "e", "me", j * step, step, [], 0)
        last = [("by", "o"), ("byf", "o")] if j == BLOCKS - 1 else []
        add(("e2", j), ("p",), {"p": 1}, "eo", "me", j * step, step, last, 0)
        add(("e3", j), ("q",), {"q": 1}, "e", "p", j * step, step, [("e2", j)], 0)
        for role, name in (("q", "e1"), ("p", "e2"), ("opp", "e3")):
            add(("d", role), ("d",), {"c": 1}, "e", role, j * step, step, [(name, j)], 0)
    add(("d", "me"), ("d",), {"c": 1}, "e", "me", 0, rows, [("by", "o")], 0)
    gather("o", 0, OWN_Z, tokens - OWN_Z, [], SLOW["o"], 1)
    for dz in (0, 1, -1, 2, -2, 3, -3, 4):
        for dy in (0, 1, -1, 2):
            deps = {0: [], 1: [("by", "o")], -1: [("by", "o")], 2: [("byf", "o")]}[dy] if dz == 0 else [("bz", "o", dy, abs(dz))]
            add(("pp", abs(dz)), ("p",), {"p": 1}, "ht", (dz, dy), kept, VIA_P, deps, 2)
    gather("p", tokens, PART_Z, kept - PART_Z, [("ph",)], SLOW["p"], 2)
    for one in m:
        one.size = one.n * 2 * (width if one.what in ("e", "eo") else depth)
    return m


def arrivals(m):
    rate = {"p": 46.0e3, "q": 46.0e3, "y": 46.0e3, "z": 46.0e3, "d": 500.0e3}
    free, when, count = {}, {}, {}
    for one in m:
        count[one.event] = count.get(one.event, 0) + 1

    def send(one, now):
        begin = max(now, free.get(one.link, 0.0))
        free[one.link] = begin + one.size / rate[one.link[0]]
        there = free[one.link] + (1.0 if one.link[0] == "d" else 2.0)
        when[one.event] = max(when.get(one.event, 0.0), there)
        count[one.event] -= 1

    initial = [one for one in m if not one.deps]
    for one in initial:
        send(one, 0.0)
    left = [one for one in m if one.deps]
    order, done = [], set()
    while any(k not in done for k in count):
        k = min((k for k in when if k not in done and not count[k]), key=lambda k: when[k])
        done.add(k)
        released = [one for one in left if done.issuperset(one.deps)]
        left = [one for one in left if one not in released]
        for one in released:
            send(one, when[k])
        order.append((k, when[k], released))
    return initial, order


def tasks(m):
    events = {one.event for one in m}
    embed = {"me": {("d", "me")}}
    for role, name in (("q", "e1"), ("p", "e2"), ("opp", "e3")):
        embed[role] = {("d", role)} | {k for k in events if k[0] == name}
    own = {k for k in events if len(k) > 1 and k[1] == "o"} | {("lab",)}
    out = [(own | embed[role], (role, 0), 2.1) for role in ROLES]
    for d in range(5):
        mine = {("pp", d)} | ({("ph",)} if d == 0 else set())
        for k in events:
            if len(k) > 1 and k[1] == "p" and k[0] != "d" and (abs(k[-1]) if k[0] not in ("by", "byf") else 0) == d:
                mine.add(k)
        out.append((mine, (d, 1), 1.25 if d in (0, 4) else 2.1))
    out.insert(ABSORB_AT, (set(), ("absorb", 0), 1.8))
    out.append((set(), ("absorb", 1), 1.8))
    return out


def program_order(m):
    initial, order = arrivals(m)
    when = {k: t - (SOONER if k[0] == "e3" else 0.0) for k, t, _ in order}
    order.sort(key=lambda entry: when[entry[0]])
    release = {k: released for k, _, released in order}
    todo, urgent = tasks(m), [k for k, _, released in order if released]
    out, waited, clock = [("send", initial)], set(), 0.0

    def wait(k):
        nonlocal clock
        clock = max(clock, when[k])
        out.append(("wait", k))
        waited.add(k)
        if release[k]:
            for dep in [dep for one in release[k] for dep in one.deps]:
                if dep not in waited:
                    wait(dep)
            out.append(("send", release[k]))
            urgent.remove(k)

    while todo or len(waited) < len(when):
        needs = todo[0][0] - waited if todo else set(when) - waited
        ready = max([when[k] for k in needs], default=0.0)
        if urgent and when[urgent[0]] <= max(clock, ready):
            wait(urgent[0])
            continue
        for k in sorted(needs, key=when.get):
            wait(k)
        if todo:
            _, task, cost = todo.pop(0)
            out.append(("matmul", task))
            clock += cost
    return out, clock


def kernel(m, steps, hid, emb, lab_hbm, token_loss, mean_loss, lab, e, eo, h, acc, top, mass, mark, sz, sp, s2, lz, lp, ly, rows, came, sent, own, tail_sent, tail_came):
    x, c = lax.axis_index("x"), lax.axis_index("c")
    z, y = lax.axis_index("z"), lax.axis_index("y")
    size = {"x": NX, "c": NC, "z": NZ, "y": NY}
    pos = {"x": x, "c": c, "z": z, "y": y}
    lines = lab_hbm.shape[0]
    tokens = lines * 128
    vocab = emb.shape[0]
    half = vocab // 2
    sign = 1 - 2 * lax.rem(x, 2)
    chip = {"me": x, "p": x + sign, "q": lax.rem(x - sign + NX, NX), "opp": lax.rem(x + 2, NX)}
    mine = lax.rem((x + 1) // 2, 2) * half
    other = half - mine

    def shifted(axis, d):
        return lax.rem(pos[axis] + (d + size[axis]), size[axis])

    def device(to):
        where = {axis: shifted(axis, d) for axis, d in to.items() if axis not in ("p", "q")}
        for role in ("p", "q"):
            if role in to:
                where["x"] = chip[role]
        return where

    def chunk_e(role):
        return chip[role] * NC + c

    def chunk_h(dz, dy):
        return shifted("z", dz) * NY + shifted("y", dy)

    own_eo = pltpu.make_async_copy(emb.at[pl.ds(pl.multiple_of(other, half), half)], eo, own.at[0])
    own_e = pltpu.make_async_copy(emb.at[pl.ds(pl.multiple_of(mine, half), half)], e.at[chunk_e("me")], own.at[1])
    own_h = pltpu.make_async_copy(hid, h.at[chunk_h(0, 0), pl.ds(0, tokens)], own.at[2])
    own_labels = pltpu.make_async_copy(lab_hbm, lab.at[0], own.at[3])
    loads = (own_h, own_labels, own_e, own_eo)
    own_h.start()

    barrier = pltpu.get_barrier_semaphore()
    near = [{"x": 1}, {"x": -1}, {"c": 1}, {"z": 1}, {"z": -1}, {"y": 1}, {"y": -1}]
    for to in near:
        pl.semaphore_signal(barrier, inc=1, device_id=device(to), device_id_type=pl.DeviceIdType.MESH)
    for one in loads[1:]:
        one.start()
    top[...] = jnp.full_like(top, -1e30)
    mass[...] = jnp.zeros_like(mass)
    mark[...] = jnp.zeros_like(mark)
    for one in loads:
        one.wait()
    pl.semaphore_wait(barrier, len(near))

    events = {}
    for one in m:
        events.setdefault(one.event, []).append(one)
    number = {event: i for i, event in enumerate(events)}

    def copy(src, dst, send_sem, recv_sem, to):
        return pltpu.make_async_remote_copy(
            src_ref=src,
            dst_ref=dst,
            send_sem=send_sem,
            recv_sem=recv_sem,
            device_id=device(to),
            device_id_type=pl.DeviceIdType.MESH,
        )

    def start_message(one):
        part = pl.ds(one.at, one.n)
        if one.what == "e":
            src = dst = e.at[chunk_e(one.where), part]
        elif one.what == "eo":
            src, dst = eo.at[part], e.at[chunk_e("me"), part]
        elif one.what == "h":
            src = dst = h.at[chunk_h(*one.where), part]
        elif one.what == "ht":
            src, dst = h.at[chunk_h(*one.where), part], h.at[chunk_h(*one.where), pl.ds(tokens + one.at, one.n)]
        else:
            src, dst = lab.at[0], lab.at[1]
        copy(src, dst, sent.at[one.group], came.at[number[one.event]], one.to).start()

    def wait_event(event):
        some = events[event]
        if some[0].what == "lab":
            ref = lab.at[1]
        else:
            ref = e if some[0].what in ("e", "eo") else h
            total = sum(one.n for one in some)
            chunks = next(k for k in range(1, 9) if total % (16 * k) == 0 and total // k <= ref.shape[1])
            ref = ref.at[pl.ds(0, chunks), pl.ds(0, total // chunks)]
        copy(ref, ref, sent.at[0], came.at[number[event]], some[0].to).wait_recv()

    first_row = (z * NY + y) * vocab + mine

    def matmul(part, token_set):
        at = pl.ds(token_set * tokens, tokens)
        if part in ROLES:
            chunks = [chip[part] * NC + i for i in range(NC)]
        else:
            chunks = [shifted("z", d) for d in sorted({part, part if part in (0, 4) else -part})]
        each = emb.shape[1] // hid.shape[1]

        def tile(i, carry):
            to = pl.ds(pl.multiple_of(i * TILE, TILE), TILE)
            left = jnp.concatenate([e[f, to] for f in chunks], axis=1)
            right = jnp.concatenate([h[f * each + i, at] for f in chunks for i in range(each)], axis=1)
            acc[to, at] += lax.dot_general(left, right, (((1,), (1,)), ((), ())), preferred_element_type=jnp.float32)
            return carry

        lax.fori_loop(0, half // TILE, tile, 0)

    def absorb(token_set):
        n = 256

        def lanes(t, carry):
            at = pl.ds(pl.multiple_of(token_set * tokens + lax.rem(t, lines) * 128, 128), 128)
            first = pl.multiple_of(t // lines * n, n)
            block = acc[pl.ds(first, n), at].reshape(n // 8, 8, 128)
            before = top[:, at]
            peak = jnp.maximum(before, jnp.max(block, axis=0))
            mass[:, at] = mass[:, at] * jnp.exp(before - peak) + jnp.sum(jnp.exp(block - peak[None]), axis=0)
            top[:, at] = peak
            row = lax.broadcasted_iota(jnp.int32, block.shape, 0) * 8 + lax.broadcasted_iota(jnp.int32, block.shape, 1)
            wanted = jnp.broadcast_to(lab[token_set, pl.ds(lax.rem(t, lines), 1)] - (first_row + first), (8, 128))
            mark[:, at] += jnp.sum(jnp.where(row == wanted[None], block, 0.0), axis=0)
            return carry

        lax.fori_loop(0, lines * (half // n), lanes, 0)

    for step in steps:
        if step[0] == "send":
            for one in step[1]:
                start_message(one)
            if not step[1][0].deps:

                def clear(i, carry):
                    acc[pl.ds(pl.multiple_of(i * 16, 16), 16)] = jnp.zeros((16, 2 * tokens), jnp.float32)
                    return carry

                lax.fori_loop(0, half // 16, clear, 0)
        elif step[0] == "wait":
            wait_event(step[1])
        else:
            if step[1][0] == "absorb":
                absorb(step[1][1])
            else:
                matmul(*step[1])

    peak = jnp.max(top[...], axis=0, keepdims=True)
    lse = peak + jnp.log(jnp.sum(mass[...] * jnp.exp(top[...] - peak), axis=0, keepdims=True))
    picked = jnp.sum(mark[...], axis=0, keepdims=True)
    slot = 2 * z
    for token_set, (to_s, to_l) in enumerate(((sz.at[slot], lz.at[slot]), (sp, lp))):
        one = [slice(token_set * tokens + t * 128, token_set * tokens + (t + 1) * 128) for t in range(lines)]
        for t in range(lines):
            to_s[t : t + 1] = lse[:, one[t]]
            to_l[t : t + 1] = picked[:, one[t]]
        to_s[lines : lines + 1] = sum(picked[:, k] for k in one)

    def combined(lse, axis):
        peak = jnp.max(lse, axis=axis, keepdims=True)
        return jnp.squeeze(peak, axis) + jnp.log(jnp.sum(jnp.exp(lse - peak), axis=axis))

    def spread(i, buffer, work):
        for src, at, to in work:
            copy(src, buffer.at[at], tail_sent.at[i], tail_came.at[i], to).start()
        all_of_them = buffer.at[pl.ds(0, len(work))]
        return copy(all_of_them, all_of_them, tail_sent.at[i], tail_came.at[i], work[0][2])

    ring = (4, 3, -3, 2, -2, 1, -1, 0)

    def along(buffer, part):
        return [w for d in ring for w in ((part, slot + 1, {"p": 1, "z": d}), (buffer.at[slot], slot, {"z": d}))][:-1]

    along_z = spread(0, sz, along(sz, sp))
    labels_z = spread(1, lz, along(lz, lp))
    along_z.wait_recv()
    me = (x * NC + c) * NY + y
    s2[me, 0:lines] = combined(sz[:, 0:lines], 0)
    s2[me, lines : lines + 1] = jnp.sum(sz[:, lines : lines + 1], axis=0)
    order = (2, 1, -1, 0)
    across = spread(2, s2, [(s2.at[me], me, {"x": i, "y": j, "c": k}) for i in order for j in order for k in (0, 1) if i or j or k])
    labels_z.wait_recv()
    ly[y] = jnp.sum(lz[...], axis=0)
    labels_y = spread(3, ly, [(ly.at[y], y, {"y": j}) for j in (2, 1, -1)])
    labels_y.wait_recv()
    across.wait_recv()
    whole = s2[...].reshape(NX * NC, NY, lines + 1, 128)
    each = jnp.sum(combined(whole[:, :, 0:lines], 1), axis=1) - jnp.sum(whole[:, :, lines], axis=1)
    mean_loss[...] = jnp.sum(jnp.sum(each, axis=0, keepdims=True), axis=1, keepdims=True) / (tokens * NX * NC)
    group = s2[pl.ds((x * NC + c) * NY, NY)]
    rows[0:lines] = combined(group[:, 0:lines], 0) - jnp.sum(ly[...], axis=0)
    rows[lines : lines + 1] = jnp.zeros((1, 128), jnp.float32)
    share = tokens // (NZ * NY)
    first = (z * NY + y) * share
    line, lane = first // 128, lax.rem(first, 128)
    two = jnp.concatenate([rows[pl.ds(line, 1)], rows[pl.ds(line + 1, 1)]], axis=1)
    two = jnp.broadcast_to(two, (8, 256))
    token_loss[...] = pltpu.roll(two, lax.rem(256 - lane, 256), 1)[0:1, 0:share]

    for group in range(4):
        some = [one for one in m if one.group == group]
        if group == 3:
            ref = lab.at[0]
        else:
            ref, n = (e, half) if group == 0 else (h, tokens)
            ref = ref.at[pl.ds(0, sum(one.n for one in some) // n), pl.ds(0, n)]
        copy(ref, ref, sent.at[group], came.at[0], some[0].to).wait_send()
    for one in (along_z, labels_z, across, labels_y):
        one.wait_send()


def body(hidden, out_embed, labels):
    tokens, depth = hidden.shape
    vocab, width = out_embed.shape
    lines = tokens // 128
    m = plan_messages(tokens, depth, vocab, width)
    steps, _ = program_order(m)
    f32 = jnp.float32
    token_loss, mean_loss = pl.pallas_call(
        functools.partial(kernel, m, steps),
        out_shape=(
            jax.ShapeDtypeStruct((1, tokens // (NZ * NY)), f32),
            jax.ShapeDtypeStruct((1, 1), f32),
        ),
        in_specs=[
            pl.BlockSpec(memory_space=pl.ANY),
            pl.BlockSpec(memory_space=pl.ANY),
            pl.BlockSpec(memory_space=pl.ANY),
        ],
        out_specs=(pl.BlockSpec(memory_space=pltpu.VMEM), pl.BlockSpec(memory_space=pltpu.VMEM)),
        scratch_shapes=[
            pltpu.VMEM((2, lines, 128), jnp.int32),
            pltpu.VMEM((NX * NC, vocab // 2, width), jnp.bfloat16),
            pltpu.VMEM((vocab // 2, width), jnp.bfloat16),
            pltpu.VMEM((NZ * NY, 2 * tokens, depth), jnp.bfloat16),
            pltpu.VMEM((vocab // 2, 2 * tokens), f32),
            pltpu.VMEM((8, 2 * tokens), f32),
            pltpu.VMEM((8, 2 * tokens), f32),
            pltpu.VMEM((8, 2 * tokens), f32),
            pltpu.VMEM((2 * NZ, lines + 1, 128), f32),
            pltpu.VMEM((lines + 1, 128), f32),
            pltpu.VMEM((NX * NC * NY, lines + 1, 128), f32),
            pltpu.VMEM((2 * NZ, lines, 128), f32),
            pltpu.VMEM((lines, 128), f32),
            pltpu.VMEM((NY, lines, 128), f32),
            pltpu.VMEM((lines + 1, 128), f32),
            pltpu.SemaphoreType.DMA((len({one.event for one in m}),)),
            pltpu.SemaphoreType.DMA((4,)),
            pltpu.SemaphoreType.DMA((4,)),
            pltpu.SemaphoreType.DMA((4,)),
            pltpu.SemaphoreType.DMA((4,)),
        ],
        compiler_params=pltpu.CompilerParams(
            collective_id=0, has_side_effects=True, vmem_limit_bytes=60 * 1024 * 1024
        ),
    )(hidden, out_embed, labels.reshape(lines, 128))
    return token_loss.reshape(-1), mean_loss.reshape(())


def solution(mesh):
    finer = Mesh(mesh.devices.reshape(NX, NC, NZ, NY), ("x", "c", "z", "y"))
    dp, tensor = ("x", "c"), ("z", "y")
    return jax.shard_map(
        body,
        mesh=finer,
        in_specs=(P(dp, tensor), P(tensor, dp), P(dp)),
        out_specs=(P(dp + tensor), P()),
        check_vma=False,
    )
```

```python
import functools

import jax
import jax.numpy as jnp
from jax import lax
from jax.experimental import pallas as pl
from jax.experimental.pallas import tpu as pltpu
from jax.sharding import Mesh
from jax.sharding import PartitionSpec as P

NX, NC, NZ, NY = 4, 2, 8, 4
BLOCKS = 4
OWN_Z, PART_Z = 480, 320
SOONER = 2.5
VIA_P = 192
TILE = 512
ABSORB_AT = 7
SLOW = {
    "o": {
        ("bz", 0): [("az", "o", 0, 2)],
        ("bz", 1): [("az", "o", 0, 2)],
        ("bz", 2): [("az", "o", 0, 1)],
    },
    "p": {
        "az": [("az", "o", 0, 4)],
        "ay": [("ay", "o", 4)],
        ("bz", 0): [("bz", "o", 0, 3)],
        ("bz", 1): [("bz", "o", 1, 3)],
        ("bz", -1): [("bz", "o", 2, 4)],
        ("bz", 2): [("bz", "o", 2, 4)],
    },
}
ROLES = ("me", "p", "q", "opp")


class Message:
    def __init__(self, event, link, to, what, where, at, n, deps, group):
        self.event, self.link, self.to, self.deps = event, link, to, deps
        self.what, self.where, self.at, self.n, self.group = what, where, at, n, group


def plan_messages(tokens, depth, vocab, width):
    m = []
    rows = vocab // 2
    step = rows // BLOCKS
    kept = tokens - VIA_P

    def add(event, link, to, what, where, at, n, deps, group):
        m.append(Message(event, link, to, what, where, at, n, deps, group))

    def gather(t, base, n_z, n_y, first, slow, group):
        def send(name, d_axis, d, where, at, n, deps):
            add(name, (d_axis, d), {d_axis: d}, "h", where, at, n, deps, group)

        at_y = base + n_z
        for d in (1, -1):
            send(("by", t), "y", d, (0, 0), at_y, n_y, first)
            send(("byf", t), "y", d, (0, -d), at_y if d == 1 else at_y + n_y // 2, n_y // 2, [("by", t)])

        def along_z(name, dy, at, n, before):
            for d in (1, -1):
                for s in range(1, 5):
                    deps = before if s == 1 else [(name, t, dy, s - 1)]
                    here, count = (at, n) if s < 4 else ((at, n // 2) if d == 1 else (at + n // 2, n // 2))
                    send((name, t, dy, s), "z", d, (-d * (s - 1), dy), here, count, deps)

        along_z("az", 0, base, n_z, first + slow.get("az", []))
        for dz in (0, 1, -1, 2, -2, 3, -3, 4):
            deps = [("az", t, 0, abs(dz))] if dz else first + slow.get("ay", [])
            for d in (1, -1):
                send(("ay", t, dz), "y", d, (dz, 0), base, n_z, deps)
            d = 1 if dz % 2 == 0 else -1
            send(("ayf", t, dz), "y", d, (dz, -d), base, n_z, [("ay", t, dz)])
        for dy in (0, 1, -1, 2):
            before = {0: first, 1: [("by", t)], -1: [("by", t)], 2: [("byf", t)]}[dy]
            along_z("bz", dy, at_y, n_y, before + slow.get(("bz", dy), []))

    add(("ph",), ("p",), {"p": 1}, "ht", (0, 0), 0, kept, [], 2)
    add(("lab",), ("p",), {"p": 1}, "lab", 0, 0, 0, [], 3)
    for j in range(BLOCKS):
        add(("e1", j), ("q",), {"q": 1}, "e", "me", j * step, step, [], 0)
        last = [("by", "o"), ("byf", "o")] if j == BLOCKS - 1 else []
        add(("e2", j), ("p",), {"p": 1}, "eo", "me", j * step, step, last, 0)
        add(("e3", j), ("q",), {"q": 1}, "e", "p", j * step, step, [("e2", j)], 0)
        for role, name in (("q", "e1"), ("p", "e2"), ("opp", "e3")):
            add(("d", role), ("d",), {"c": 1}, "e", role, j * step, step, [(name, j)], 0)
    add(("d", "me"), ("d",), {"c": 1}, "e", "me", 0, rows, [("by", "o")], 0)
    gather("o", 0, OWN_Z, tokens - OWN_Z, [], SLOW["o"], 1)
    for dz in (0, 1, -1, 2, -2, 3, -3, 4):
        for dy in (0, 1, -1, 2):
            deps = {0: [], 1: [("by", "o")], -1: [("by", "o")], 2: [("byf", "o")]}[dy] if dz == 0 else [("bz", "o", dy, abs(dz))]
            add(("pp", abs(dz)), ("p",), {"p": 1}, "ht", (dz, dy), kept, VIA_P, deps, 2)
    gather("p", tokens, PART_Z, kept - PART_Z, [("ph",)], SLOW["p"], 2)
    for one in m:
        one.size = one.n * 2 * (width if one.what in ("e", "eo") else depth)
    return m


def arrivals(m):
    rate = {"p": 46.0e3, "q": 46.0e3, "y": 46.0e3, "z": 46.0e3, "d": 500.0e3}
    free, when, count = {}, {}, {}
    for one in m:
        count[one.event] = count.get(one.event, 0) + 1

    def send(one, now):
        begin = max(now, free.get(one.link, 0.0))
        free[one.link] = begin + one.size / rate[one.link[0]]
        there = free[one.link] + (1.0 if one.link[0] == "d" else 2.0)
        when[one.event] = max(when.get(one.event, 0.0), there)
        count[one.event] -= 1

    initial = [one for one in m if not one.deps]
    for one in initial:
        send(one, 0.0)
    left = [one for one in m if one.deps]
    order, done = [], set()
    while any(k not in done for k in count):
        k = min((k for k in when if k not in done and not count[k]), key=lambda k: when[k])
        done.add(k)
        released = [one for one in left if done.issuperset(one.deps)]
        left = [one for one in left if one not in released]
        for one in released:
            send(one, when[k])
        order.append((k, when[k], released))
    return initial, order


def tasks(m):
    events = {one.event for one in m}
    embed = {"me": {("d", "me")}}
    for role, name in (("q", "e1"), ("p", "e2"), ("opp", "e3")):
        embed[role] = {("d", role)} | {k for k in events if k[0] == name}
    own = {k for k in events if len(k) > 1 and k[1] == "o"} | {("lab",)}
    out = [(own | embed[role], (role, 0), 2.1) for role in ROLES]
    for d in range(5):
        mine = {("pp", d)} | ({("ph",)} if d == 0 else set())
        for k in events:
            if len(k) > 1 and k[1] == "p" and k[0] != "d" and (abs(k[-1]) if k[0] not in ("by", "byf") else 0) == d:
                mine.add(k)
        out.append((mine, (d, 1), 1.25 if d in (0, 4) else 2.1))
    out.insert(ABSORB_AT, (set(), ("absorb", 0), 1.8))
    out.append((set(), ("absorb", 1), 1.8))
    return out


def program_order(m):
    initial, order = arrivals(m)
    when = {k: t - (SOONER if k[0] == "e3" else 0.0) for k, t, _ in order}
    order.sort(key=lambda entry: when[entry[0]])
    release = {k: released for k, _, released in order}
    todo, urgent = tasks(m), [k for k, _, released in order if released]
    out, waited, clock = [("send", initial)], set(), 0.0

    def wait(k):
        nonlocal clock
        clock = max(clock, when[k])
        out.append(("wait", k))
        waited.add(k)
        if release[k]:
            for dep in [dep for one in release[k] for dep in one.deps]:
                if dep not in waited:
                    wait(dep)
            out.append(("send", release[k]))
            urgent.remove(k)

    while todo or len(waited) < len(when):
        needs = todo[0][0] - waited if todo else set(when) - waited
        ready = max([when[k] for k in needs], default=0.0)
        if urgent and when[urgent[0]] <= max(clock, ready):
            wait(urgent[0])
            continue
        for k in sorted(needs, key=when.get):
            wait(k)
        if todo:
            _, task, cost = todo.pop(0)
            out.append(("matmul", task))
            clock += cost
    return out, clock


def kernel(m, steps, hid, emb, lab_hbm, token_loss, mean_loss, lab, e, eo, h, acc, top, mass, mark, sz, sp, s2, lz, lp, ly, rows, came, sent, own, tail_sent, tail_came):
    x, c = lax.axis_index("x"), lax.axis_index("c")
    z, y = lax.axis_index("z"), lax.axis_index("y")
    size = {"x": NX, "c": NC, "z": NZ, "y": NY}
    pos = {"x": x, "c": c, "z": z, "y": y}
    lines = lab_hbm.shape[0]
    tokens = lines * 128
    vocab = emb.shape[0]
    half = vocab // 2
    sign = 1 - 2 * lax.rem(x, 2)
    chip = {"me": x, "p": x + sign, "q": lax.rem(x - sign + NX, NX), "opp": lax.rem(x + 2, NX)}
    mine = lax.rem((x + 1) // 2, 2) * half
    other = half - mine

    def shifted(axis, d):
        return lax.rem(pos[axis] + (d + size[axis]), size[axis])

    def device(to):
        where = {axis: shifted(axis, d) for axis, d in to.items() if axis not in ("p", "q")}
        for role in ("p", "q"):
            if role in to:
                where["x"] = chip[role]
        return where

    def chunk_e(role):
        return chip[role] * NC + c

    def chunk_h(dz, dy):
        return shifted("z", dz) * NY + shifted("y", dy)

    own_eo = pltpu.make_async_copy(emb.at[pl.ds(pl.multiple_of(other, half), half)], eo, own.at[0])
    own_e = pltpu.make_async_copy(emb.at[pl.ds(pl.multiple_of(mine, half), half)], e.at[chunk_e("me")], own.at[1])
    own_h = pltpu.make_async_copy(hid, h.at[chunk_h(0, 0), pl.ds(0, tokens)], own.at[2])
    own_labels = pltpu.make_async_copy(lab_hbm, lab.at[0], own.at[3])
    loads = (own_h, own_labels, own_e, own_eo)
    own_h.start()

    barrier = pltpu.get_barrier_semaphore()
    near = [{"x": 1}, {"x": -1}, {"c": 1}, {"z": 1}, {"z": -1}, {"y": 1}, {"y": -1}]
    for to in near:
        pl.semaphore_signal(barrier, inc=1, device_id=device(to), device_id_type=pl.DeviceIdType.MESH)
    for one in loads[1:]:
        one.start()
    top[...] = jnp.full_like(top, -1e30)
    mass[...] = jnp.zeros_like(mass)
    mark[...] = jnp.zeros_like(mark)
    own_h.wait()
    own_labels.wait()
    pl.semaphore_wait(barrier, len(near))

    events = {}
    for one in m:
        events.setdefault(one.event, []).append(one)
    number = {event: i for i, event in enumerate(events)}

    def copy(src, dst, send_sem, recv_sem, to):
        return pltpu.make_async_remote_copy(
            src_ref=src,
            dst_ref=dst,
            send_sem=send_sem,
            recv_sem=recv_sem,
            device_id=device(to),
            device_id_type=pl.DeviceIdType.MESH,
        )

    def start_message(one):
        part = pl.ds(one.at, one.n)
        if one.what == "e":
            src = dst = e.at[chunk_e(one.where), part]
        elif one.what == "eo":
            src, dst = eo.at[part], e.at[chunk_e("me"), part]
        elif one.what == "h":
            src = dst = h.at[chunk_h(*one.where), part]
        elif one.what == "ht":
            src, dst = h.at[chunk_h(*one.where), part], h.at[chunk_h(*one.where), pl.ds(tokens + one.at, one.n)]
        else:
            src, dst = lab.at[0], lab.at[1]
        copy(src, dst, sent.at[one.group], came.at[number[one.event]], one.to).start()

    def wait_event(event):
        some = events[event]
        if some[0].what == "lab":
            ref = lab.at[1]
        else:
            ref = e if some[0].what in ("e", "eo") else h
            total = sum(one.n for one in some)
            chunks = next(k for k in range(1, 9) if total % (16 * k) == 0 and total // k <= ref.shape[1])
            ref = ref.at[pl.ds(0, chunks), pl.ds(0, total // chunks)]
        copy(ref, ref, sent.at[0], came.at[number[event]], some[0].to).wait_recv()

    first_row = (z * NY + y) * vocab + mine

    def matmul(part, token_set):
        at = pl.ds(token_set * tokens, tokens)
        if part in ROLES:
            chunks = [chip[part] * NC + i for i in range(NC)]
        else:
            chunks = [shifted("z", d) for d in sorted({part, part if part in (0, 4) else -part})]
        each = emb.shape[1] // hid.shape[1]

        def tile(i, carry):
            to = pl.ds(pl.multiple_of(i * TILE, TILE), TILE)
            left = jnp.concatenate([e[f, to] for f in chunks], axis=1)
            right = jnp.concatenate([h[f * each + i, at] for f in chunks for i in range(each)], axis=1)
            acc[to, at] += lax.dot_general(left, right, (((1,), (1,)), ((), ())), preferred_element_type=jnp.float32)
            return carry

        lax.fori_loop(0, half // TILE, tile, 0)

    def absorb(token_set):
        n = 256

        def lanes(t, carry):
            at = pl.ds(pl.multiple_of(token_set * tokens + lax.rem(t, lines) * 128, 128), 128)
            first = pl.multiple_of(t // lines * n, n)
            block = acc[pl.ds(first, n), at].reshape(n // 8, 8, 128)
            before = top[:, at]
            peak = jnp.maximum(before, jnp.max(block, axis=0))
            mass[:, at] = mass[:, at] * jnp.exp(before - peak) + jnp.sum(jnp.exp(block - peak[None]), axis=0)
            top[:, at] = peak
            row = lax.broadcasted_iota(jnp.int32, block.shape, 0) * 8 + lax.broadcasted_iota(jnp.int32, block.shape, 1)
            wanted = jnp.broadcast_to(lab[token_set, pl.ds(lax.rem(t, lines), 1)] - (first_row + first), (8, 128))
            mark[:, at] += jnp.sum(jnp.where(row == wanted[None], block, 0.0), axis=0)
            return carry

        lax.fori_loop(0, lines * (half // n), lanes, 0)

    for step in steps:
        if step[0] == "send":
            first = not step[1][0].deps
            now = [one for one in step[1] if not first or one.what not in ("e", "eo")]
            for one in now:
                start_message(one)
            if first:
                own_e.wait()
                own_eo.wait()
                for one in step[1]:
                    if one not in now:
                        start_message(one)

                def clear(i, carry):
                    acc[pl.ds(pl.multiple_of(i * 16, 16), 16)] = jnp.zeros((16, 2 * tokens), jnp.float32)
                    return carry

                lax.fori_loop(0, half // 16, clear, 0)
        elif step[0] == "wait":
            wait_event(step[1])
        else:
            if step[1][0] == "absorb":
                absorb(step[1][1])
            else:
                matmul(*step[1])

    peak = jnp.max(top[...], axis=0, keepdims=True)
    lse = peak + jnp.log(jnp.sum(mass[...] * jnp.exp(top[...] - peak), axis=0, keepdims=True))
    picked = jnp.sum(mark[...], axis=0, keepdims=True)
    slot = 2 * z
    for token_set, (to_s, to_l) in enumerate(((sz.at[slot], lz.at[slot]), (sp, lp))):
        one = [slice(token_set * tokens + t * 128, token_set * tokens + (t + 1) * 128) for t in range(lines)]
        for t in range(lines):
            to_s[t : t + 1] = lse[:, one[t]]
            to_l[t : t + 1] = picked[:, one[t]]
        to_s[lines : lines + 1] = sum(picked[:, k] for k in one)

    def combined(lse, axis):
        peak = jnp.max(lse, axis=axis, keepdims=True)
        return jnp.squeeze(peak, axis) + jnp.log(jnp.sum(jnp.exp(lse - peak), axis=axis))

    def spread(i, buffer, work):
        for src, at, to in work:
            copy(src, buffer.at[at], tail_sent.at[i], tail_came.at[i], to).start()
        all_of_them = buffer.at[pl.ds(0, len(work))]
        return copy(all_of_them, all_of_them, tail_sent.at[i], tail_came.at[i], work[0][2])

    ring = (4, 3, -3, 2, -2, 1, -1, 0)

    def along(buffer, part):
        return [w for d in ring for w in ((part, slot + 1, {"p": 1, "z": d}), (buffer.at[slot], slot, {"z": d}))][:-1]

    along_z = spread(0, sz, along(sz, sp))
    labels_z = spread(1, lz, along(lz, lp))
    along_z.wait_recv()
    me = (x * NC + c) * NY + y
    s2[me, 0:lines] = combined(sz[:, 0:lines], 0)
    s2[me, lines : lines + 1] = jnp.sum(sz[:, lines : lines + 1], axis=0)
    order = (2, 1, -1, 0)
    across = spread(2, s2, [(s2.at[me], me, {"x": i, "y": j, "c": k}) for i in order for j in order for k in (0, 1) if i or j or k])
    labels_z.wait_recv()
    ly[y] = jnp.sum(lz[...], axis=0)
    labels_y = spread(3, ly, [(ly.at[y], y, {"y": j}) for j in (2, 1, -1)])
    labels_y.wait_recv()
    across.wait_recv()
    whole = s2[...].reshape(NX * NC, NY, lines + 1, 128)
    each = jnp.sum(combined(whole[:, :, 0:lines], 1), axis=1) - jnp.sum(whole[:, :, lines], axis=1)
    mean_loss[...] = jnp.sum(jnp.sum(each, axis=0, keepdims=True), axis=1, keepdims=True) / (tokens * NX * NC)
    group = s2[pl.ds((x * NC + c) * NY, NY)]
    rows[0:lines] = combined(group[:, 0:lines], 0) - jnp.sum(ly[...], axis=0)
    rows[lines : lines + 1] = jnp.zeros((1, 128), jnp.float32)
    share = tokens // (NZ * NY)
    first = (z * NY + y) * share
    line, lane = first // 128, lax.rem(first, 128)
    two = jnp.concatenate([rows[pl.ds(line, 1)], rows[pl.ds(line + 1, 1)]], axis=1)
    two = jnp.broadcast_to(two, (8, 256))
    token_loss[...] = pltpu.roll(two, lax.rem(256 - lane, 256), 1)[0:1, 0:share]

    for group in range(4):
        some = [one for one in m if one.group == group]
        if group == 3:
            ref = lab.at[0]
        else:
            ref, n = (e, half) if group == 0 else (h, tokens)
            ref = ref.at[pl.ds(0, sum(one.n for one in some) // n), pl.ds(0, n)]
        copy(ref, ref, sent.at[group], came.at[0], some[0].to).wait_send()
    for one in (along_z, labels_z, across, labels_y):
        one.wait_send()


def body(hidden, out_embed, labels):
    tokens, depth = hidden.shape
    vocab, width = out_embed.shape
    lines = tokens // 128
    m = plan_messages(tokens, depth, vocab, width)
    steps, _ = program_order(m)
    f32 = jnp.float32
    token_loss, mean_loss = pl.pallas_call(
        functools.partial(kernel, m, steps),
        out_shape=(
            jax.ShapeDtypeStruct((1, tokens // (NZ * NY)), f32),
            jax.ShapeDtypeStruct((1, 1), f32),
        ),
        in_specs=[
            pl.BlockSpec(memory_space=pl.ANY),
            pl.BlockSpec(memory_space=pl.ANY),
            pl.BlockSpec(memory_space=pl.ANY),
        ],
        out_specs=(pl.BlockSpec(memory_space=pltpu.VMEM), pl.BlockSpec(memory_space=pltpu.VMEM)),
        scratch_shapes=[
            pltpu.VMEM((2, lines, 128), jnp.int32),
            pltpu.VMEM((NX * NC, vocab // 2, width), jnp.bfloat16),
            pltpu.VMEM((vocab // 2, width), jnp.bfloat16),
            pltpu.VMEM((NZ * NY, 2 * tokens, depth), jnp.bfloat16),
            pltpu.VMEM((vocab // 2, 2 * tokens), f32),
            pltpu.VMEM((8, 2 * tokens), f32),
            pltpu.VMEM((8, 2 * tokens), f32),
            pltpu.VMEM((8, 2 * tokens), f32),
            pltpu.VMEM((2 * NZ, lines + 1, 128), f32),
            pltpu.VMEM((lines + 1, 128), f32),
            pltpu.VMEM((NX * NC * NY, lines + 1, 128), f32),
            pltpu.VMEM((2 * NZ, lines, 128), f32),
            pltpu.VMEM((lines, 128), f32),
            pltpu.VMEM((NY, lines, 128), f32),
            pltpu.VMEM((lines + 1, 128), f32),
            pltpu.SemaphoreType.DMA((len({one.event for one in m}),)),
            pltpu.SemaphoreType.DMA((4,)),
            pltpu.SemaphoreType.DMA((4,)),
            pltpu.SemaphoreType.DMA((4,)),
            pltpu.SemaphoreType.DMA((4,)),
        ],
        compiler_params=pltpu.CompilerParams(
            collective_id=0, has_side_effects=True, vmem_limit_bytes=60 * 1024 * 1024
        ),
    )(hidden, out_embed, labels.reshape(lines, 128))
    return token_loss.reshape(-1), mean_loss.reshape(())


def solution(mesh):
    finer = Mesh(mesh.devices.reshape(NX, NC, NZ, NY), ("x", "c", "z", "y"))
    dp, tensor = ("x", "c"), ("z", "y")
    return jax.shard_map(
        body,
        mesh=finer,
        in_specs=(P(dp, tensor), P(tensor, dp), P(dp)),
        out_specs=(P(dp + tensor), P()),
        check_vma=False,
    )
```
